32 devices in a mesh: dp: 16 (over z, y, x), comp: 2 (over core).
Axes of the slice: x: 2, y: 2, z: 4, core: 2. Of those that a mesh axis runs over, the one named last changes fastest.
Arguments:
- events: float32 [32768, 32], P(('dp', 'comp')), may hold values from -60 to 60
- means: float32 [64, 32], replicated, may hold values from -4 to 4
- factors: float32 [64, 32, 32], replicated, may hold values from -1.5 to 1.6, as said below
- log_weights: float32 [64], replicated, may hold values from -4 to 4
Outputs:
- new_means: float32 [64, 32], replicated
- new_factors: float32 [64, 32, 32], replicated
- new_log_weights: float32 [64], replicated
- event_loglik: float32 [32768], P(('dp', 'comp'))
The draws below stay inside these ranges and needn't reach their ends.
Inputs may be any that keep to these rules, and one draw needn't show every extreme that they name: Each factors[k] is lower triangular with diagonal entries between 0.6 and 1.6.
All inputs are finite; a program needn't handle non-finite values.
Results may differ from the reference program's by a relative error of at most 0.0009.
Values sent between devices are 32-bit elements; how exact they have to be, the bound alone decides.
No kernel may reach another device: no remote copies, remote signals or barrier semaphores. Data moves between devices by JAX's collectives and lax.ppermute only.
A program may use at most 64 MiB of HBM per device.

```python
import math
import jax
import jax.numpy as jnp
from jax import lax

K = 64
D = 32
ITERS = 2
EVENTS = 32768


def draw_events(key, part):
    base = jax.random.normal(jax.random.fold_in(key, 11), (EVENTS, D), jnp.float32)
    values = 1.5 * base
    return jnp.clip(values, -60.0, 60.0)


def draw_factors(key, part):
    lower_part = 0.25 * jax.random.normal(jax.random.fold_in(key, 21), (K, D, D), jnp.float32)
    lower_part = jnp.clip(lower_part, -1.5, 1.5)
    diag_vals = jnp.exp(jax.random.uniform(jax.random.fold_in(key, 22), (K, D), jnp.float32, -0.5108, 0.47))
    strict = jnp.tril(lower_part, -1)
    return strict + diag_vals[:, :, None] * jnp.eye(D, dtype=jnp.float32)[None, :, :]


def noise(rng, shape, spread, bound, kind=jnp.bfloat16):
    values = jax.random.normal(rng, shape, jnp.float32) * spread
    return jnp.minimum(jnp.maximum(values, -bound), bound).astype(kind)


def setup_inputs(seed: int = 0) -> dict:
    streams_of = jax.random.split(jax.random.key(seed), 5)
    events = draw_events(jax.random.fold_in(streams_of[4], 71), 0)
    means = noise(streams_of[1], (K, D), 1.0, 4.0, jnp.float32)
    factors = draw_factors(jax.random.fold_in(streams_of[4], 71), 0)
    log_weights = noise(streams_of[3], (K,), 1.0, 4.0, jnp.float32)
    return {"events": events, "means": means, "factors": factors, "log_weights": log_weights}


ridge = 0.1
prior_count = 1.0
highest = lax.Precision.HIGHEST

def block_stats(events_block, means, factors, log_weights):
    comp_count, width = means.shape
    block_rows = events_block.shape[0]
    project = factors.reshape(comp_count * width, width).T
    offset = jnp.einsum('kij,kj->ki', factors, means, precision=highest).reshape(-1)
    diag_part = jnp.diagonal(factors, axis1=1, axis2=2)
    constant = log_weights - jax.nn.logsumexp(log_weights) + jnp.sum(jnp.log(diag_part), axis=1) - 0.5 * width * math.log(2.0 * math.pi)
    shifted = jnp.dot(events_block.astype(jnp.float32), project.astype(jnp.float32), precision=highest, preferred_element_type=jnp.float32) - offset
    quadratic = jnp.sum((shifted * shifted).reshape(block_rows, comp_count, width), axis=2)
    log_dens = constant[None, :] - 0.5 * quadratic
    row_max = jnp.max(log_dens, axis=1, keepdims=True)
    loglik = row_max[:, 0] + jnp.log(jnp.sum(jnp.exp(log_dens - row_max), axis=1))
    respons = jnp.exp(log_dens - loglik[:, None])
    counts = jnp.sum(respons, axis=0)
    centered = events_block[:, None, :] - means[None, :, :]
    weighted = (respons[:, :, None] * centered).reshape(block_rows, comp_count * width)
    first = jnp.sum(weighted, axis=0)
    second = lax.dot_general(weighted.astype(jnp.float32), events_block.astype(jnp.float32), (((0,), (0,)), ((), ())), precision=highest, preferred_element_type=jnp.float32)
    return (loglik, counts, first, second)

def update(counts, first, second, means, comp_total, event_total):
    comp_count, width = means.shape
    denom = counts + prior_count
    first_mat = first.reshape(comp_count, width)
    second_mat = second.reshape(comp_count, width, width)
    new_means = means + first_mat / denom[:, None]
    scatter = second_mat - first_mat[:, :, None] * means[:, None, :] - first_mat[:, :, None] * first_mat[:, None, :] / denom[:, None, None]
    scatter = 0.5 * (scatter + jnp.swapaxes(scatter, 1, 2))
    identity = jnp.eye(width, dtype=jnp.float32)
    covar = (scatter + ridge * identity) / denom[:, None, None]
    lower = jnp.linalg.cholesky(covar)
    new_factors = jax.scipy.linalg.solve_triangular(lower, jnp.broadcast_to(identity, lower.shape), lower=True)
    new_logw = jnp.log(denom / (event_total + comp_total * prior_count))
    return (new_means, new_factors, new_logw)

def reference(events, means, factors, log_weights):
    event_total = events.shape[0]
    block_size = min(2048, event_total)
    blocks = events.reshape(event_total // block_size, block_size, events.shape[1])
    comp_count, width = means.shape
    loglik = jnp.zeros((event_total,), jnp.float32)
    for turn in range(ITERS):

        def one_block(carry, events_block, means=means, factors=factors, log_weights=log_weights):
            block_ll, counts, first, second = block_stats(events_block, means, factors, log_weights)
            return ((carry[0] + counts, carry[1] + first, carry[2] + second), block_ll)
        start = (jnp.zeros((comp_count,), jnp.float32), jnp.zeros((comp_count * width,), jnp.float32), jnp.zeros((comp_count * width, width), jnp.float32))
        totals, loglik_blocks = lax.scan(one_block, start, blocks)
        loglik = loglik_blocks.reshape(-1)
        means, factors, log_weights = update(totals[0], totals[1], totals[2], means, comp_count, event_total)
    return (means, factors, log_weights, loglik)
```

```python
import functools
import math

import jax
import jax.numpy as jnp
from jax import lax
from jax.experimental import pallas as pl
from jax.experimental.pallas import tpu as pltpu
from jax.sharding import PartitionSpec as P

ITERS = 2
SUB = 8
LANES = 128

ridge = 0.1
prior_count = 1.0


def split3(value):
    high = value.astype(jnp.bfloat16)
    rest = value - high.astype(jnp.float32)
    mid = rest.astype(jnp.bfloat16)
    low = (rest - mid.astype(jnp.float32)).astype(jnp.bfloat16)
    return high, mid, low


def block_pairs(width):
    blocks = width // SUB
    return [(b, c) for b in range(blocks) for c in range(b, blocks)]


def moment_rows(width):
    used = len(block_pairs(width)) * SUB * SUB + width
    step = 4 * SUB * 2
    return -(-(used + 1) // step) * step


def local_moments(x_ref, proj_ref, mu, logw, loglik_ref, mom_ref, gain_ref, quad_ref, feat_ref, yt_ref):
    rows, width = x_ref.shape
    comps = mu.shape[1]
    cols = width * comps
    proj = proj_ref[...]
    reps = cols // LANES

    mu_wide = jnp.concatenate([mu] * (LANES // comps), axis=1)
    sub_id = lax.broadcasted_iota(jnp.int32, (width, LANES), 0)
    lane_id = lax.broadcasted_iota(jnp.int32, (width, LANES), 1) // comps
    log_det = jnp.zeros((1, LANES), jnp.float32)
    offsets = []
    for t in range(reps):
        tile = proj[:, t * LANES : (t + 1) * LANES]
        offsets.append(jnp.sum(tile * mu_wide, axis=0, keepdims=True))
        row_of = lane_id + t * (LANES // comps)
        diag = jnp.sum(jnp.where(sub_id == row_of, tile, 0.0), axis=0, keepdims=True)
        log_det = log_det + jnp.log(diag)
    offset = jnp.concatenate(offsets, axis=1)

    logw_max = jnp.max(logw, axis=1, keepdims=True)
    logw_lse = logw_max + jnp.log(jnp.sum(jnp.exp(logw - logw_max), axis=1, keepdims=True))
    constant = logw - logw_lse - 0.5 * width * math.log(2.0 * math.pi)
    start = -2.0 * (
        log_det + jnp.concatenate([constant] + [jnp.zeros_like(constant)] * (LANES // comps - 1), axis=1)
    )

    p1, p2, p3 = split3(proj)
    for place, part in enumerate((p1, p2, p3, p1, p2, p1)):
        gain_ref[place * width : (place + 1) * width, :] = part
    depth = gain_ref.shape[0]
    tail = depth - 6 * width
    o1, o2, o3 = (part.astype(jnp.float32) for part in split3(-offset))
    tail_id = lax.broadcasted_iota(jnp.int32, (tail, cols), 0)
    tail_rows = jnp.where(
        tail_id == 0, o1, jnp.where(tail_id == 1, o2, jnp.where(tail_id == 2, o3, 0.0))
    )
    gain_ref[6 * width :, :] = tail_rows.astype(jnp.bfloat16)

    x = x_ref[...]
    group = LANES // width
    x_wide = jnp.concatenate([x] * group, axis=1)
    x1, x2, x3 = (part.astype(jnp.float32) for part in split3(x_wide))
    lane = lax.broadcasted_iota(jnp.int32, (rows, LANES), 1)
    first_half = jnp.where(lane < 3 * width, x1, x2)
    second_half = jnp.where(
        lane < width, x2, jnp.where(lane < 2 * width, x3, jnp.where(lane < 2 * width + 3, 1.0, 0.0))
    )
    streamed = jnp.concatenate([first_half, second_half], axis=1).astype(jnp.bfloat16)

    quad_ref[...] = jnp.broadcast_to(start, (rows, LANES))
    tile_cols = 2 * LANES
    for t in range(cols // tile_cols):
        z = jnp.dot(
            streamed,
            gain_ref[:, t * tile_cols : (t + 1) * tile_cols],
            preferred_element_type=jnp.float32,
        )
        quad_ref[...] += z[:, :LANES] * z[:, :LANES] + z[:, LANES:] * z[:, LANES:]

    quad_t = quad_ref[...].T
    total = quad_t[:comps]
    for part in range(1, LANES // comps):
        total = total + quad_t[part * comps : (part + 1) * comps]
    log_dens = -0.5 * total
    peak = jnp.max(log_dens, axis=0, keepdims=True)
    weight = jnp.exp(log_dens - peak)
    norm = jnp.sum(weight, axis=0, keepdims=True)
    loglik = peak + jnp.log(norm)
    for line in range(rows // LANES):
        loglik_ref[line : line + 1, :] = loglik[:, line * LANES : (line + 1) * LANES]
    respons = weight / norm
    resp_parts = jnp.concatenate(split3(respons), axis=0)

    center = jnp.mean(mu, axis=1, keepdims=True)
    yt_ref[...] = x.T - center
    total_rows = feat_ref.shape[0] // 3

    def put(base, value):
        for place, part in enumerate(split3(value)):
            at = place * total_rows + base
            feat_ref[at : at + value.shape[0], :] = part

    base = 0
    for b, c in block_pairs(width):
        right = yt_ref[c * SUB : (c + 1) * SUB, :]
        for i in range(0, SUB, 2):
            left0 = yt_ref[b * SUB + i : b * SUB + i + 1, :]
            left1 = yt_ref[b * SUB + i + 1 : b * SUB + i + 2, :]
            put(base, jnp.concatenate([left0 * right, left1 * right], axis=0))
            base += 2 * SUB
    put(base, yt_ref[...])
    base += width
    put(base, jnp.ones((total_rows - base, rows), jnp.float32))

    sums = lax.dot_general(
        feat_ref[...],
        resp_parts,
        (((1,), (1,)), ((), ())),
        preferred_element_type=jnp.float32,
    )
    sums = sums[:total_rows] + sums[total_rows : 2 * total_rows] + sums[2 * total_rows :]
    sums = sums[:, :comps] + sums[:, comps : 2 * comps] + sums[:, 2 * comps :]
    folds = LANES // comps
    part_rows = total_rows // folds
    packed = jnp.concatenate(
        [sums[place * part_rows : (place + 1) * part_rows] for place in range(folds)], axis=1
    )
    half = mom_ref.shape[1]
    for place in range(mom_ref.shape[0]):
        mom_ref[place] = packed[place * half : (place + 1) * half]


def update(mom_ref, mu, event_total):
    width, comps = mu.shape
    blocks = width // SUB
    packed = jnp.concatenate([mom_ref[place] for place in range(mom_ref.shape[0])], axis=0)
    sums = jnp.concatenate(
        [packed[:, place * comps : (place + 1) * comps] for place in range(LANES // comps)], axis=0
    )
    pairs = block_pairs(width)
    base = len(pairs) * SUB * SUB
    about = sums[base : base + width]
    counts = sums[base + width : base + width + 1]

    shift = mu - jnp.mean(mu, axis=1, keepdims=True)
    first = about - counts * shift
    denom = counts + prior_count
    step = first / denom
    new_mu = mu + step
    new_logw = jnp.log(denom / (event_total + comps * prior_count))

    def block(value, b):
        return value[b * SUB : (b + 1) * SUB]

    def row(value, i):
        return jnp.broadcast_to(value[i : i + 1], (SUB, comps))

    sub_id = lax.broadcasted_iota(jnp.int32, (SUB, comps), 0)
    cov = [dict() for _ in range(width)]
    for place, (b, c) in enumerate(pairs):
        for i in range(SUB):
            at = b * SUB + i
            raw = sums[(place * SUB + i) * SUB : (place * SUB + i + 1) * SUB]
            value = raw - (
                row(about, at) * block(shift, c)
                + row(shift, at) * block(first, c)
                + row(first, at) * block(step, c)
            )
            if b == c:
                value = value + jnp.where(sub_id == i, ridge, 0.0)
            cov[at][c] = value

    inverse = [
        {i // SUB: jnp.where(sub_id == i % SUB, 1.0, 0.0).astype(jnp.float32)} for i in range(width)
    ]
    factors = []
    for p in range(width):
        b = p // SUB
        pivot = cov[p][b][p % SUB : p % SUB + 1]
        recip = jnp.broadcast_to(1.0 / pivot, (SUB, comps))
        scaled = {c: cov[p][c] * recip for c in range(b, blocks)}
        for i in range(p + 1, width):
            factor = row(scaled[i // SUB], i % SUB)
            for c in range(i // SUB, blocks):
                cov[i][c] = cov[i][c] - factor * cov[p][c]
            for c in range(b + 1):
                change = factor * inverse[p][c]
                inverse[i][c] = inverse[i][c] - change if c in inverse[i] else -change
        scale = jnp.broadcast_to(jnp.sqrt(denom / pivot), (SUB, comps))
        zero = jnp.zeros((SUB, comps), jnp.float32)
        factors.append(
            jnp.concatenate(
                [inverse[p][c] * scale if c in inverse[p] else zero for c in range(blocks)], axis=0
            )
        )
    return new_mu, factors, new_logw


def first_kernel(x_ref, proj_ref, mu_ref, logw_ref, loglik_ref, mom_ref, *scratch):
    local_moments(x_ref, proj_ref, mu_ref[...], logw_ref[...], loglik_ref, mom_ref, *scratch)


def middle_kernel(
    event_total, x_ref, summed_ref, mu_ref, loglik_ref, mom_ref, new_mu_ref, proj_ref, *scratch
):
    mu, factors, logw = update(summed_ref, mu_ref[...], event_total)
    new_mu_ref[...] = mu
    group = LANES // mu.shape[1]
    for t in range(len(factors) // group):
        proj_ref[:, t * LANES : (t + 1) * LANES] = jnp.concatenate(
            factors[t * group : (t + 1) * group], axis=1
        )
    local_moments(x_ref, proj_ref, mu, logw, loglik_ref, mom_ref, *scratch)


def last_kernel(event_total, summed_ref, mu_ref, new_mu_ref, factor_ref, logw_ref):
    mu, factors, logw = update(summed_ref, mu_ref[...], event_total)
    new_mu_ref[...] = mu
    logw_ref[...] = logw
    for i, value in enumerate(factors):
        factor_ref[i] = value


def group_steps(size):
    steps, stride = [], 1
    while size > 1:
        radix = 4 if size % 4 == 0 else (2 if size % 2 == 0 else size)
        steps.append((stride, radix))
        stride *= radix
        size //= radix
    return steps


def peer(index, stride, radix, shift):
    digit = index // stride % radix
    other = digit ^ shift if radix & (radix - 1) == 0 else (digit + shift) % radix
    return index + (other - digit) * stride


def all_sum(moments):
    cores = lax.axis_size("comp")
    size = lax.axis_size("dp")
    core = lax.axis_index("comp")
    swap = [(0, 1), (1, 0)]
    mine = lax.dynamic_index_in_dim(moments, core, 0, keepdims=False)
    other = lax.dynamic_index_in_dim(moments, 1 - core, 0, keepdims=False)
    mine = mine + lax.ppermute(other, "comp", swap)
    for stride, radix in group_steps(size):
        order = sorted(range(1, radix), key=lambda shift: -bin(shift).count("1"))
        received = [
            lax.ppermute(mine, "dp", [(i, peer(i, stride, radix, shift)) for i in range(size)])
            for shift in order
        ]
        for value in received:
            mine = mine + value
    theirs = lax.ppermute(mine, "comp", swap)
    return jnp.where(core == 0, jnp.stack([mine, theirs]), jnp.stack([theirs, mine]))


def body(events, means, factors, log_weights):
    rows, width = events.shape
    comps = means.shape[0]
    event_total = rows * lax.axis_size("dp") * lax.axis_size("comp")
    cols = width * comps
    f32 = jnp.float32

    total_rows = moment_rows(width)
    halves = lax.axis_size("comp")
    mom_shape = jax.ShapeDtypeStruct((halves, total_rows * comps // LANES // halves, LANES), f32)
    loglik_shape = jax.ShapeDtypeStruct((rows // LANES, LANES), f32)
    mu_shape = jax.ShapeDtypeStruct((width, comps), f32)
    scratch = [
        pltpu.VMEM((2 * LANES, cols), jnp.bfloat16),
        pltpu.VMEM((rows, LANES), f32),
        pltpu.VMEM((3 * total_rows, rows), jnp.bfloat16),
        pltpu.VMEM((width, rows), f32),
    ]
    params = pltpu.CompilerParams(vmem_limit_bytes=56 * 1024 * 1024)

    proj = factors.transpose(2, 1, 0).reshape(width, cols)
    mu = means.T
    logw = log_weights.reshape(1, comps)
    loglik, moments = pl.pallas_call(
        first_kernel,
        out_shape=(loglik_shape, mom_shape),
        scratch_shapes=scratch,
        compiler_params=params,
        name="first",
    )(events, proj, mu, logw)
    for _ in range(1, ITERS):
        loglik, moments, mu = pl.pallas_call(
            functools.partial(middle_kernel, event_total),
            out_shape=(loglik_shape, mom_shape, mu_shape),
            scratch_shapes=[pltpu.VMEM((width, cols), f32)] + scratch,
            compiler_params=params,
            name="middle",
        )(events, all_sum(moments), mu)
    mu, new_factors, logw = pl.pallas_call(
        functools.partial(last_kernel, event_total),
        out_shape=(
            mu_shape,
            jax.ShapeDtypeStruct((width, width, comps), f32),
            jax.ShapeDtypeStruct((1, comps), f32),
        ),
        compiler_params=params,
        name="last",
    )(all_sum(moments), mu)
    return mu.T, new_factors.transpose(2, 0, 1), logw.reshape(comps), loglik.reshape(rows)


def solution(mesh):
    in_specs = (P(("dp", "comp"), None), P(), P(), P())
    out_specs = (P(), P(), P(), P(("dp", "comp")))
    return jax.shard_map(body, mesh=mesh, in_specs=in_specs, out_specs=out_specs, check_vma=False)
```

```python
import functools
import math

import jax
import jax.numpy as jnp
from jax import lax
from jax.experimental import pallas as pl
from jax.experimental.pallas import tpu as pltpu
from jax.sharding import PartitionSpec as P

ITERS = 2
SUB = 8
LANES = 128

ridge = 0.1
prior_count = 1.0


def split3(value):
    high = value.astype(jnp.bfloat16)
    rest = value - high.astype(jnp.float32)
    mid = rest.astype(jnp.bfloat16)
    low = (rest - mid.astype(jnp.float32)).astype(jnp.bfloat16)
    return high, mid, low


def upper_pairs(width):
    blocks = width // SUB
    return [(b, c) for b in range(blocks) for c in range(b + 1, blocks)]


def diagonal_pairs(width):
    return [(b, b + 1) for b in range(0, width // SUB, 2)]


def moment_layout(width):
    diagonal = len(upper_pairs(width)) * SUB * SUB
    linear = diagonal + len(diagonal_pairs(width)) * SUB * (SUB + 1)
    ones = linear + width
    step = 4 * SUB * 2
    return diagonal, linear, ones, -(-(ones + 1) // step) * step


def local_moments(
    xt_ref, proj_ref, mu, logw, loglik_ref, mine_ref, other_ref, gain_ref, quad_ref, feat_ref, yt_ref
):
    width, rows = xt_ref.shape
    comps = mu.shape[1]
    cols = width * comps
    proj = proj_ref[...]
    reps = cols // LANES

    mu_wide = jnp.concatenate([mu] * (LANES // comps), axis=1)
    sub_id = lax.broadcasted_iota(jnp.int32, (width, LANES), 0)
    lane_id = lax.broadcasted_iota(jnp.int32, (width, LANES), 1) // comps
    log_det = jnp.zeros((1, LANES), jnp.float32)
    offsets = []
    for t in range(reps):
        tile = proj[:, t * LANES : (t + 1) * LANES]
        offsets.append(jnp.sum(tile * mu_wide, axis=0, keepdims=True))
        row_of = lane_id + t * (LANES // comps)
        diag = jnp.sum(jnp.where(sub_id == row_of, tile, 0.0), axis=0, keepdims=True)
        log_det = log_det + jnp.log(diag)
    offset = jnp.concatenate(offsets, axis=1)

    logw_max = jnp.max(logw, axis=1, keepdims=True)
    logw_lse = logw_max + jnp.log(jnp.sum(jnp.exp(logw - logw_max), axis=1, keepdims=True))
    constant = logw - logw_lse - 0.5 * width * math.log(2.0 * math.pi)
    start = -2.0 * (
        log_det + jnp.concatenate([constant] + [jnp.zeros_like(constant)] * (LANES // comps - 1), axis=1)
    )

    p1, p2, p3 = split3(proj)
    for place, part in enumerate((p1, p2, p3, p1, p2, p1)):
        gain_ref[place * width : (place + 1) * width, :] = part
    depth = gain_ref.shape[0]
    tail = depth - 6 * width
    o1, o2, o3 = (part.astype(jnp.float32) for part in split3(-offset))
    tail_id = lax.broadcasted_iota(jnp.int32, (tail, cols), 0)
    tail_rows = jnp.where(
        tail_id == 0, o1, jnp.where(tail_id == 1, o2, jnp.where(tail_id == 2, o3, 0.0))
    )
    gain_ref[6 * width :, :] = tail_rows.astype(jnp.bfloat16)

    x = xt_ref[...].T
    group = LANES // width
    x_wide = jnp.concatenate([x] * group, axis=1)
    x1, x2, x3 = (part.astype(jnp.float32) for part in split3(x_wide))
    lane = lax.broadcasted_iota(jnp.int32, (rows, LANES), 1)
    first_half = jnp.where(lane < 3 * width, x1, x2)
    second_half = jnp.where(
        lane < width, x2, jnp.where(lane < 2 * width, x3, jnp.where(lane < 2 * width + 3, 1.0, 0.0))
    )
    streamed = jnp.concatenate([first_half, second_half], axis=1).astype(jnp.bfloat16)

    quad_ref[...] = jnp.broadcast_to(start, (rows, LANES))
    tile_cols = 2 * LANES
    for t in range(cols // tile_cols):
        z = jnp.dot(
            streamed,
            gain_ref[:, t * tile_cols : (t + 1) * tile_cols],
            preferred_element_type=jnp.float32,
        )
        quad_ref[...] += z[:, :LANES] * z[:, :LANES] + z[:, LANES:] * z[:, LANES:]

    quad_t = quad_ref[...].T
    total = quad_t[:comps]
    for part in range(1, LANES // comps):
        total = total + quad_t[part * comps : (part + 1) * comps]
    log_dens = -0.5 * total
    peak = jnp.max(log_dens, axis=0, keepdims=True)
    weight = jnp.exp(log_dens - peak)
    norm = jnp.sum(weight, axis=0, keepdims=True)
    loglik = peak + jnp.log(norm)
    for line in range(rows // LANES):
        loglik_ref[line : line + 1, :] = loglik[:, line * LANES : (line + 1) * LANES]
    respons = weight / norm
    resp_parts = jnp.concatenate(split3(respons), axis=0)

    center = jnp.mean(mu, axis=1, keepdims=True)
    yt_ref[...] = xt_ref[...] - center
    total_rows = feat_ref.shape[0] // 3

    def put(base, value):
        for place, part in enumerate(split3(value)):
            at = place * total_rows + base
            feat_ref[at : at + value.shape[0], :] = part

    products = []

    def product(i, c):
        return yt_ref[i : i + 1, :] * yt_ref[c * SUB : (c + 1) * SUB, :]

    for b, c in upper_pairs(width):
        products += [product(b * SUB + i, c) for i in range(SUB)]
    sub = lax.broadcasted_iota(jnp.int32, (SUB, rows), 0)
    for b, c in diagonal_pairs(width):
        products.append(product(b * SUB, b))
        for i in range(1, SUB):
            products.append(
                jnp.where(sub >= i, product(b * SUB + i, b), product(c * SUB + i - 1, c))
            )
        products.append(product(c * SUB + SUB - 1, c))
    for at in range(0, len(products), 2):
        put(at * SUB, jnp.concatenate(products[at : at + 2], axis=0))
    _, linear, ones, _ = moment_layout(width)
    put(linear, yt_ref[...])
    put(ones, jnp.ones((total_rows - ones, rows), jnp.float32))

    sums = lax.dot_general(
        feat_ref[...],
        resp_parts,
        (((1,), (1,)), ((), ())),
        preferred_element_type=jnp.float32,
    )
    sums = sums[:total_rows] + sums[total_rows : 2 * total_rows] + sums[2 * total_rows :]
    sums = sums[:, :comps] + sums[:, comps : 2 * comps] + sums[:, 2 * comps :]
    folds = LANES // comps
    part_rows = total_rows // folds
    packed = jnp.concatenate(
        [sums[place * part_rows : (place + 1) * part_rows] for place in range(folds)], axis=1
    )
    half = mine_ref.shape[0]
    core = lax.axis_index("comp")
    lower, upper = packed[:half], packed[half:]
    mine_ref[...] = jnp.where(core == 0, lower, upper)
    other_ref[...] = jnp.where(core == 0, upper, lower)


def update(mine_ref, theirs_ref, mu, event_total):
    width, comps = mu.shape
    blocks = width // SUB
    core = lax.axis_index("comp")
    mine, theirs = mine_ref[...], theirs_ref[...]
    packed = jnp.concatenate(
        [jnp.where(core == 0, mine, theirs), jnp.where(core == 0, theirs, mine)], axis=0
    )
    sums = jnp.concatenate(
        [packed[:, place * comps : (place + 1) * comps] for place in range(LANES // comps)], axis=0
    )
    diagonal, linear, ones, _ = moment_layout(width)
    about = sums[linear : linear + width]
    counts = sums[ones : ones + 1]

    shift = mu - jnp.mean(mu, axis=1, keepdims=True)
    first = about - counts * shift
    denom = counts + prior_count
    step = first / denom
    new_mu = mu + step
    new_logw = jnp.log(denom / (event_total + comps * prior_count))

    def block(value, b):
        return value[b * SUB : (b + 1) * SUB]

    def row(value, i):
        return jnp.broadcast_to(value[i : i + 1], (SUB, comps))

    sub_id = lax.broadcasted_iota(jnp.int32, (SUB, comps), 0)
    def register(place):
        return sums[place * SUB : (place + 1) * SUB]

    raw = {}
    for place, (b, c) in enumerate(upper_pairs(width)):
        for i in range(SUB):
            raw[b * SUB + i, c] = register(place * SUB + i)
    for place, (b, c) in enumerate(diagonal_pairs(width)):
        shared = [register(diagonal // SUB + place * (SUB + 1) + i) for i in range(SUB + 1)]
        for i in range(SUB):
            raw[b * SUB + i, b] = shared[i]
            value = shared[i + 1]
            for j in range(i + 1, SUB):
                value = jnp.where(sub_id == j, row(shared[j + 1], i), value)
            raw[c * SUB + i, c] = value

    cov = [dict() for _ in range(width)]
    for (at, c), value in raw.items():
        value = value - (
            row(about, at) * block(shift, c)
            + row(shift, at) * block(first, c)
            + row(first, at) * block(step, c)
        )
        if at // SUB == c:
            value = value + jnp.where(sub_id == at % SUB, ridge, 0.0)
        cov[at][c] = value

    inverse = [
        {i // SUB: jnp.where(sub_id == i % SUB, 1.0, 0.0).astype(jnp.float32)} for i in range(width)
    ]
    factors = []
    for p in range(width):
        b = p // SUB
        pivot = cov[p][b][p % SUB : p % SUB + 1]
        recip = jnp.broadcast_to(1.0 / pivot, (SUB, comps))
        scaled = {c: cov[p][c] * recip for c in range(b, blocks)}
        for i in range(p + 1, width):
            factor = row(scaled[i // SUB], i % SUB)
            for c in range(i // SUB, blocks):
                cov[i][c] = cov[i][c] - factor * cov[p][c]
            for c in range(b + 1):
                change = factor * inverse[p][c]
                inverse[i][c] = inverse[i][c] - change if c in inverse[i] else -change
        scale = jnp.broadcast_to(jnp.sqrt(denom / pivot), (SUB, comps))
        zero = jnp.zeros((SUB, comps), jnp.float32)
        factors.append(
            jnp.concatenate(
                [inverse[p][c] * scale if c in inverse[p] else zero for c in range(blocks)], axis=0
            )
        )
    return new_mu, factors, new_logw


def place_factors(proj_ref, rows_of, comps):
    group = LANES // comps
    for t in range(len(rows_of) // group):
        proj_ref[:, t * LANES : (t + 1) * LANES] = jnp.concatenate(
            rows_of[t * group : (t + 1) * group], axis=1
        )


def first_kernel(
    xt_ref, factor_ref, mu_ref, logw_ref, loglik_ref, mine_ref, other_ref, proj_ref, *scratch
):
    width, _, comps = factor_ref.shape
    place_factors(proj_ref, [factor_ref[i] for i in range(width)], comps)
    local_moments(
        xt_ref, proj_ref, mu_ref[...], logw_ref[...], loglik_ref, mine_ref, other_ref, *scratch
    )


def middle_kernel(
    event_total,
    xt_ref,
    mine_ref,
    theirs_ref,
    mu_ref,
    loglik_ref,
    new_mine_ref,
    new_other_ref,
    new_mu_ref,
    proj_ref,
    *scratch,
):
    mu, factors, logw = update(mine_ref, theirs_ref, mu_ref[...], event_total)
    new_mu_ref[...] = mu
    place_factors(proj_ref, factors, mu.shape[1])
    local_moments(xt_ref, proj_ref, mu, logw, loglik_ref, new_mine_ref, new_other_ref, *scratch)


def last_kernel(event_total, mine_ref, theirs_ref, mu_ref, new_mu_ref, factor_ref, logw_ref):
    mu, factors, logw = update(mine_ref, theirs_ref, mu_ref[...], event_total)
    new_mu_ref[...] = mu
    logw_ref[...] = logw
    for i, value in enumerate(factors):
        factor_ref[i] = value


def group_steps(size):
    steps, stride = [], 1
    while size > 1:
        radix = 4 if size % 4 == 0 else (2 if size % 2 == 0 else size)
        steps.append((stride, radix))
        stride *= radix
        size //= radix
    return steps


def peer(index, stride, radix, shift):
    digit = index // stride % radix
    other = digit ^ shift if radix & (radix - 1) == 0 else (digit + shift) % radix
    return index + (other - digit) * stride


def all_sum(mine, other):
    size = lax.axis_size("dp")
    swap = [(0, 1), (1, 0)]
    mine = mine + lax.ppermute(other, "comp", swap)
    for stride, radix in group_steps(size):
        order = sorted(range(1, radix), key=lambda shift: -bin(shift).count("1"))
        received = [
            lax.ppermute(mine, "dp", [(i, peer(i, stride, radix, shift)) for i in range(size)])
            for shift in order
        ]
        for value in received:
            mine = mine + value
    return mine, lax.ppermute(mine, "comp", swap)


def body(events, means, factors, log_weights):
    rows, width = events.shape
    comps = means.shape[0]
    event_total = rows * lax.axis_size("dp") * lax.axis_size("comp")
    cols = width * comps
    f32 = jnp.float32

    total_rows = moment_layout(width)[-1]
    halves = lax.axis_size("comp")
    mom_shape = jax.ShapeDtypeStruct((total_rows * comps // LANES // halves, LANES), f32)
    loglik_shape = jax.ShapeDtypeStruct((rows // LANES, LANES), f32)
    mu_shape = jax.ShapeDtypeStruct((width, comps), f32)
    scratch = [
        pltpu.VMEM((width, cols), f32),
        pltpu.VMEM((2 * LANES, cols), jnp.bfloat16),
        pltpu.VMEM((rows, LANES), f32),
        pltpu.VMEM((3 * total_rows, rows), jnp.bfloat16),
        pltpu.VMEM((width, rows), f32),
    ]
    params = pltpu.CompilerParams(vmem_limit_bytes=24 * 1024 * 1024)

    xt = events.T
    mu = means.T
    loglik, mine, other = pl.pallas_call(
        first_kernel,
        out_shape=(loglik_shape, mom_shape, mom_shape),
        scratch_shapes=scratch,
        compiler_params=params,
        name="first",
    )(xt, factors.transpose(1, 2, 0), mu, log_weights.reshape(1, comps))
    for _ in range(1, ITERS):
        loglik, mine, other, mu = pl.pallas_call(
            functools.partial(middle_kernel, event_total),
            out_shape=(loglik_shape, mom_shape, mom_shape, mu_shape),
            scratch_shapes=scratch,
            compiler_params=params,
            name="middle",
        )(xt, *all_sum(mine, other), mu)
    mu, new_factors, logw = pl.pallas_call(
        functools.partial(last_kernel, event_total),
        out_shape=(
            mu_shape,
            jax.ShapeDtypeStruct((width, width, comps), f32),
            jax.ShapeDtypeStruct((1, comps), f32),
        ),
        compiler_params=params,
        name="last",
    )(*all_sum(mine, other), mu)
    return mu.T, new_factors.transpose(2, 0, 1), logw.reshape(comps), loglik.reshape(rows)


def solution(mesh):
    in_specs = (P(("dp", "comp"), None), P(), P(), P())
    out_specs = (P(), P(), P(), P(("dp", "comp")))
    return jax.shard_map(body, mesh=mesh, in_specs=in_specs, out_specs=out_specs, check_vma=False)
```

```python
import functools
import math

import jax
import jax.numpy as jnp
from jax import lax
from jax.experimental import pallas as pl
from jax.experimental.pallas import tpu as pltpu
from jax.sharding import PartitionSpec as P

ITERS = 2
SUB = 8
LANES = 128

ridge = 0.1
prior_count = 1.0


def split3(value):
    high = value.astype(jnp.bfloat16)
    rest = value - high.astype(jnp.float32)
    mid = rest.astype(jnp.bfloat16)
    low = (rest - mid.astype(jnp.float32)).astype(jnp.bfloat16)
    return high, mid, low


def upper_pairs(width):
    blocks = width // SUB
    return [(b, c) for b in range(blocks) for c in range(b + 1, blocks)]


def diagonal_pairs(width):
    return [(b, b + 1) for b in range(0, width // SUB, 2)]


def moment_layout(width):
    diagonal = len(upper_pairs(width)) * SUB * SUB
    linear = diagonal + len(diagonal_pairs(width)) * SUB * (SUB + 1)
    ones = linear + width
    step = 4 * SUB * 2
    return diagonal, linear, ones, -(-(ones + 1) // step) * step


def local_moments(
    xt_ref, proj_ref, mu, logw, loglik_ref, mine_ref, other_ref, gain_ref, quad_ref, feat_ref, yt_ref
):
    width, rows = xt_ref.shape
    comps = mu.shape[1]
    cols = width * comps
    proj = proj_ref[...]
    reps = cols // LANES

    mu_wide = jnp.concatenate([mu] * (LANES // comps), axis=1)
    sub_id = lax.broadcasted_iota(jnp.int32, (width, LANES), 0)
    lane_id = lax.broadcasted_iota(jnp.int32, (width, LANES), 1) // comps
    log_det = jnp.zeros((1, LANES), jnp.float32)
    offsets = []
    for t in range(reps):
        tile = proj[:, t * LANES : (t + 1) * LANES]
        offsets.append(jnp.sum(tile * mu_wide, axis=0, keepdims=True))
        row_of = lane_id + t * (LANES // comps)
        diag = jnp.sum(jnp.where(sub_id == row_of, tile, 0.0), axis=0, keepdims=True)
        log_det = log_det + jnp.log(diag)
    offset = jnp.concatenate(offsets, axis=1)

    logw_max = jnp.max(logw, axis=1, keepdims=True)
    logw_lse = logw_max + jnp.log(jnp.sum(jnp.exp(logw - logw_max), axis=1, keepdims=True))
    constant = logw - logw_lse - 0.5 * width * math.log(2.0 * math.pi)
    start = -2.0 * (
        log_det + jnp.concatenate([constant] + [jnp.zeros_like(constant)] * (LANES // comps - 1), axis=1)
    )

    p1, p2, p3 = split3(proj)
    for place, part in enumerate((p1, p2, p3, p1, p2, p1)):
        gain_ref[place * width : (place + 1) * width, :] = part
    depth = gain_ref.shape[0]
    tail = depth - 6 * width
    o1, o2, o3 = (part.astype(jnp.float32) for part in split3(-offset))
    tail_id = lax.broadcasted_iota(jnp.int32, (tail, cols), 0)
    tail_rows = jnp.where(
        tail_id == 0, o1, jnp.where(tail_id == 1, o2, jnp.where(tail_id == 2, o3, 0.0))
    )
    gain_ref[6 * width :, :] = tail_rows.astype(jnp.bfloat16)

    x = xt_ref[...].T
    group = LANES // width
    x_wide = jnp.concatenate([x] * group, axis=1)
    x1, x2, x3 = (part.astype(jnp.float32) for part in split3(x_wide))
    lane = lax.broadcasted_iota(jnp.int32, (rows, LANES), 1)
    first_half = jnp.where(lane < 3 * width, x1, x2)
    second_half = jnp.where(
        lane < width, x2, jnp.where(lane < 2 * width, x3, jnp.where(lane < 2 * width + 3, 1.0, 0.0))
    )
    streamed = jnp.concatenate([first_half, second_half], axis=1).astype(jnp.bfloat16)

    quad_ref[...] = jnp.broadcast_to(start, (rows, LANES))
    tile_cols = 2 * LANES
    for t in range(cols // tile_cols):
        z = jnp.dot(
            streamed,
            gain_ref[:, t * tile_cols : (t + 1) * tile_cols],
            preferred_element_type=jnp.float32,
        )
        quad_ref[...] += z[:, :LANES] * z[:, :LANES] + z[:, LANES:] * z[:, LANES:]

    quad_t = quad_ref[...].T
    total = quad_t[:comps]
    for part in range(1, LANES // comps):
        total = total + quad_t[part * comps : (part + 1) * comps]
    log_dens = -0.5 * total
    peak = jnp.max(log_dens, axis=0, keepdims=True)
    weight = jnp.exp(log_dens - peak)
    norm = jnp.sum(weight, axis=0, keepdims=True)
    loglik = peak + jnp.log(norm)
    for line in range(rows // LANES):
        loglik_ref[line : line + 1, :] = loglik[:, line * LANES : (line + 1) * LANES]
    respons = weight / norm
    resp_parts = jnp.concatenate(split3(respons), axis=0)

    center = jnp.mean(mu, axis=1, keepdims=True)
    yt_ref[...] = xt_ref[...] - center
    total_rows = feat_ref.shape[0] // 3

    def put(base, value):
        for place, part in enumerate(split3(value)):
            at = place * total_rows + base
            feat_ref[at : at + value.shape[0], :] = part

    products = []

    def product(i, c):
        return yt_ref[i : i + 1, :] * yt_ref[c * SUB : (c + 1) * SUB, :]

    for b, c in upper_pairs(width):
        products += [product(b * SUB + i, c) for i in range(SUB)]
    sub = lax.broadcasted_iota(jnp.int32, (SUB, rows), 0)
    for b, c in diagonal_pairs(width):
        products.append(product(b * SUB, b))
        for i in range(1, SUB):
            products.append(
                jnp.where(sub >= i, product(b * SUB + i, b), product(c * SUB + i - 1, c))
            )
        products.append(product(c * SUB + SUB - 1, c))
    for at in range(0, len(products), 2):
        put(at * SUB, jnp.concatenate(products[at : at + 2], axis=0))
    _, linear, ones, _ = moment_layout(width)
    put(linear, yt_ref[...])
    put(ones, jnp.ones((total_rows - ones, rows), jnp.float32))

    sums = lax.dot_general(
        feat_ref[...],
        resp_parts,
        (((1,), (1,)), ((), ())),
        preferred_element_type=jnp.float32,
    )
    sums = sums[:total_rows] + sums[total_rows : 2 * total_rows] + sums[2 * total_rows :]
    sums = sums[:, :comps] + sums[:, comps : 2 * comps] + sums[:, 2 * comps :]
    folds = LANES // comps
    part_rows = total_rows // folds
    packed = jnp.concatenate(
        [sums[place * part_rows : (place + 1) * part_rows] for place in range(folds)], axis=1
    )
    half = mine_ref.shape[0]
    core = lax.axis_index("comp")
    lower, upper = packed[:half], packed[half:]
    mine_ref[...] = jnp.where(core == 0, lower, upper)
    other_ref[...] = jnp.where(core == 0, upper, lower)


def update(mine_ref, theirs_ref, mu, event_total, emit=None):
    width, comps = mu.shape
    blocks = width // SUB
    core = lax.axis_index("comp")
    mine, theirs = mine_ref[...], theirs_ref[...]
    packed = jnp.concatenate(
        [jnp.where(core == 0, mine, theirs), jnp.where(core == 0, theirs, mine)], axis=0
    )
    sums = jnp.concatenate(
        [packed[:, place * comps : (place + 1) * comps] for place in range(LANES // comps)], axis=0
    )
    diagonal, linear, ones, _ = moment_layout(width)
    about = sums[linear : linear + width]
    counts = sums[ones : ones + 1]

    shift = mu - jnp.mean(mu, axis=1, keepdims=True)
    first = about - counts * shift
    denom = counts + prior_count
    step = first / denom
    new_mu = mu + step
    new_logw = jnp.log(denom / (event_total + comps * prior_count))

    def block(value, b):
        return value[b * SUB : (b + 1) * SUB]

    def row(value, i):
        return jnp.broadcast_to(value[i : i + 1], (SUB, comps))

    sub_id = lax.broadcasted_iota(jnp.int32, (SUB, comps), 0)
    def register(place):
        return sums[place * SUB : (place + 1) * SUB]

    raw = {}
    for place, (b, c) in enumerate(upper_pairs(width)):
        for i in range(SUB):
            raw[b * SUB + i, c] = register(place * SUB + i)
    for place, (b, c) in enumerate(diagonal_pairs(width)):
        shared = [register(diagonal // SUB + place * (SUB + 1) + i) for i in range(SUB + 1)]
        for i in range(SUB):
            raw[b * SUB + i, b] = shared[i]
            value = shared[i + 1]
            for j in range(i + 1, SUB):
                value = jnp.where(sub_id == j, row(shared[j + 1], i), value)
            raw[c * SUB + i, c] = value

    cov = [dict() for _ in range(width)]
    for (at, c), value in raw.items():
        value = value - (
            row(about, at) * block(shift, c)
            + row(shift, at) * block(first, c)
            + row(first, at) * block(step, c)
        )
        if at // SUB == c:
            value = value + jnp.where(sub_id == at % SUB, ridge, 0.0)
        cov[at][c] = value

    inverse = [
        {i // SUB: jnp.where(sub_id == i % SUB, 1.0, 0.0).astype(jnp.float32)} for i in range(width)
    ]
    factors = []
    for p in range(width):
        b = p // SUB
        pivot = cov[p][b][p % SUB : p % SUB + 1]
        recip = jnp.broadcast_to(1.0 / pivot, (SUB, comps))
        scaled = {c: cov[p][c] * recip for c in range(b, blocks)}
        for i in range(p + 1, width):
            factor = row(scaled[i // SUB], i % SUB)
            for c in range(i // SUB, blocks):
                cov[i][c] = cov[i][c] - factor * cov[p][c]
            for c in range(b + 1):
                change = factor * inverse[p][c]
                inverse[i][c] = inverse[i][c] - change if c in inverse[i] else -change
        scale = jnp.broadcast_to(jnp.sqrt(denom / pivot), (SUB, comps))
        zero = jnp.zeros((SUB, comps), jnp.float32)
        factors.append(
            jnp.concatenate(
                [inverse[p][c] * scale if c in inverse[p] else zero for c in range(blocks)], axis=0
            )
        )
        if emit is not None:
            emit(p, factors[p])
    return new_mu, factors, new_logw


def place_factors(proj_ref, rows_of, comps):
    group = LANES // comps
    for t in range(len(rows_of) // group):
        proj_ref[:, t * LANES : (t + 1) * LANES] = jnp.concatenate(
            rows_of[t * group : (t + 1) * group], axis=1
        )


def first_kernel(
    xt_hbm,
    factor_hbm,
    mu_hbm,
    logw_hbm,
    loglik_ref,
    mine_ref,
    other_ref,
    xt_ref,
    sems,
    proj_ref,
    factor_ref,
    mu_ref,
    logw_ref,
    *scratch,
):
    pairs = ((factor_hbm, factor_ref), (mu_hbm, mu_ref), (logw_hbm, logw_ref), (xt_hbm, xt_ref))
    copies = [
        pltpu.make_async_copy(source, target, sems.at[place])
        for place, (source, target) in enumerate(pairs)
    ]
    for copy in copies:
        copy.start()
    for copy in copies:
        copy.wait()
    width, _, comps = factor_ref.shape
    place_factors(proj_ref, [factor_ref[i] for i in range(width)], comps)
    local_moments(
        xt_ref, proj_ref, mu_ref[...], logw_ref[...], loglik_ref, mine_ref, other_ref, *scratch
    )


def middle_kernel(
    event_total,
    xt_ref,
    mine_ref,
    theirs_ref,
    mu_ref,
    loglik_ref,
    new_mine_ref,
    new_other_ref,
    new_mu_ref,
    proj_ref,
    *scratch,
):
    mu, factors, logw = update(mine_ref, theirs_ref, mu_ref[...], event_total)
    new_mu_ref[...] = mu
    place_factors(proj_ref, factors, mu.shape[1])
    local_moments(xt_ref, proj_ref, mu, logw, loglik_ref, new_mine_ref, new_other_ref, *scratch)


def last_kernel(
    event_total, mine_ref, theirs_ref, mu_ref, new_mu_ref, factor_hbm, logw_ref, factor_ref, sems
):
    width = factor_ref.shape[0]
    copies = []

    def emit(i, value):
        factor_ref[i] = value
        if i % SUB == SUB - 1:
            rows_of = pl.ds(i + 1 - SUB, SUB)
            copy = pltpu.make_async_copy(
                factor_ref.at[rows_of], factor_hbm.at[rows_of], sems.at[i // SUB]
            )
            copy.start()
            copies.append(copy)

    mu, _, logw = update(mine_ref, theirs_ref, mu_ref[...], event_total, emit)
    new_mu_ref[...] = mu
    logw_ref[...] = logw
    for copy in copies:
        copy.wait()


def group_steps(size):
    steps, stride = [], 1
    while size > 1:
        radix = 4 if size % 4 == 0 else (2 if size % 2 == 0 else size)
        steps.append((stride, radix))
        stride *= radix
        size //= radix
    return steps


def peer(index, stride, radix, shift):
    digit = index // stride % radix
    other = digit ^ shift if radix & (radix - 1) == 0 else (digit + shift) % radix
    return index + (other - digit) * stride


def all_sum(mine, other):
    size = lax.axis_size("dp")
    swap = [(0, 1), (1, 0)]
    mine = mine + lax.ppermute(other, "comp", swap)
    for stride, radix in group_steps(size):
        order = list(range(1, radix)) if stride == 1 else [*range(2, radix), 1]
        received = [
            lax.ppermute(mine, "dp", [(i, peer(i, stride, radix, shift)) for i in range(size)])
            for shift in order
        ]
        for value in received:
            mine = mine + value
    return mine, lax.ppermute(mine, "comp", swap)


def body(events, means, factors, log_weights):
    rows, width = events.shape
    comps = means.shape[0]
    event_total = rows * lax.axis_size("dp") * lax.axis_size("comp")
    cols = width * comps
    f32 = jnp.float32

    total_rows = moment_layout(width)[-1]
    halves = lax.axis_size("comp")
    mom_shape = jax.ShapeDtypeStruct((total_rows * comps // LANES // halves, LANES), f32)
    loglik_shape = jax.ShapeDtypeStruct((rows // LANES, LANES), f32)
    mu_shape = jax.ShapeDtypeStruct((width, comps), f32)
    scratch = [
        pltpu.VMEM((width, cols), f32),
        pltpu.VMEM((2 * LANES, cols), jnp.bfloat16),
        pltpu.VMEM((rows, LANES), f32),
        pltpu.VMEM((3 * total_rows, rows), jnp.bfloat16),
        pltpu.VMEM((width, rows), f32),
    ]
    load = [pltpu.VMEM((width, rows), f32), pltpu.SemaphoreType.DMA((4,))]
    params = pltpu.CompilerParams(vmem_limit_bytes=24 * 1024 * 1024)
    in_hbm = pl.BlockSpec(memory_space=pltpu.HBM)
    in_vmem = pl.BlockSpec(memory_space=pltpu.VMEM)

    xt = events.T
    mu = means.T
    inputs = (xt, factors.transpose(1, 2, 0), mu, log_weights.reshape(1, comps))
    loglik, mine, other = pl.pallas_call(
        first_kernel,
        out_shape=(loglik_shape, mom_shape, mom_shape),
        in_specs=[in_hbm] * 4,
        scratch_shapes=load
        + scratch[:1]
        + [
            pltpu.VMEM((width, width, comps), f32),
            pltpu.VMEM((width, comps), f32),
            pltpu.VMEM((1, comps), f32),
        ]
        + scratch[1:],
        compiler_params=params,
        name="first",
    )(*(pltpu.with_memory_space_constraint(value, pltpu.HBM) for value in inputs))
    for _ in range(1, ITERS):
        loglik, mine, other, mu = pl.pallas_call(
            functools.partial(middle_kernel, event_total),
            out_shape=(loglik_shape, mom_shape, mom_shape, mu_shape),
            scratch_shapes=scratch,
            compiler_params=params,
            name="middle",
        )(xt, *all_sum(mine, other), mu)
    mu, new_factors, logw = pl.pallas_call(
        functools.partial(last_kernel, event_total),
        out_shape=(
            mu_shape,
            jax.ShapeDtypeStruct((width, width, comps), f32),
            jax.ShapeDtypeStruct((1, comps), f32),
        ),
        out_specs=(in_vmem, in_hbm, in_vmem),
        scratch_shapes=[
            pltpu.VMEM((width, width, comps), f32),
            pltpu.SemaphoreType.DMA((width // SUB,)),
        ],
        compiler_params=params,
        name="last",
    )(*all_sum(mine, other), mu)
    return mu.T, new_factors.transpose(2, 0, 1), logw.reshape(comps), loglik.reshape(rows)


def solution(mesh):
    in_specs = (P(("dp", "comp"), None), P(), P(), P())
    out_specs = (P(), P(), P(), P(("dp", "comp")))
    return jax.shard_map(body, mesh=mesh, in_specs=in_specs, out_specs=out_specs, check_vma=False)
```

```python
import functools
import math

import jax
import jax.numpy as jnp
from jax import lax
from jax.experimental import pallas as pl
from jax.experimental.pallas import tpu as pltpu
from jax.sharding import PartitionSpec as P

ITERS = 2
SUB = 8
LANES = 128

ridge = 0.1
prior_count = 1.0


def split3(value):
    high = value.astype(jnp.bfloat16)
    rest = value - high.astype(jnp.float32)
    mid = rest.astype(jnp.bfloat16)
    low = (rest - mid.astype(jnp.float32)).astype(jnp.bfloat16)
    return high, mid, low


def upper_pairs(width):
    blocks = width // SUB
    return [(b, c) for b in range(blocks) for c in range(b + 1, blocks)]


def diagonal_pairs(width):
    return [(b, b + 1) for b in range(0, width // SUB, 2)]


def moment_layout(width):
    diagonal = len(upper_pairs(width)) * SUB * SUB
    linear = diagonal + len(diagonal_pairs(width)) * SUB * (SUB + 1)
    ones = linear + width
    step = 4 * SUB * 2
    return diagonal, linear, ones, -(-(ones + 1) // step) * step


def local_moments(
    xt_ref, proj_ref, mu, logw, loglik_ref, mine_ref, other_ref, gain_ref, quad_ref, feat_ref, yt_ref
):
    width, rows = xt_ref.shape
    comps = mu.shape[1]
    cols = width * comps
    proj = proj_ref[...]
    reps = cols // LANES

    mu_wide = jnp.concatenate([mu] * (LANES // comps), axis=1)
    sub_id = lax.broadcasted_iota(jnp.int32, (width, LANES), 0)
    lane_id = lax.broadcasted_iota(jnp.int32, (width, LANES), 1) // comps
    log_det = jnp.zeros((1, LANES), jnp.float32)
    offsets = []
    for t in range(reps):
        tile = proj[:, t * LANES : (t + 1) * LANES]
        offsets.append(jnp.sum(tile * mu_wide, axis=0, keepdims=True))
        row_of = lane_id + t * (LANES // comps)
        diag = jnp.sum(jnp.where(sub_id == row_of, tile, 0.0), axis=0, keepdims=True)
        log_det = log_det + jnp.log(diag)
    offset = jnp.concatenate(offsets, axis=1)

    logw_max = jnp.max(logw, axis=1, keepdims=True)
    logw_lse = logw_max + jnp.log(jnp.sum(jnp.exp(logw - logw_max), axis=1, keepdims=True))
    constant = logw - logw_lse - 0.5 * width * math.log(2.0 * math.pi)
    start = -2.0 * (
        log_det + jnp.concatenate([constant] + [jnp.zeros_like(constant)] * (LANES // comps - 1), axis=1)
    )

    p1, p2, p3 = split3(proj)
    for place, part in enumerate((p1, p2, p3, p1, p2, p1)):
        gain_ref[place * width : (place + 1) * width, :] = part
    depth = gain_ref.shape[0]
    tail = depth - 6 * width
    o1, o2, o3 = (part.astype(jnp.float32) for part in split3(-offset))
    tail_id = lax.broadcasted_iota(jnp.int32, (tail, cols), 0)
    tail_rows = jnp.where(
        tail_id == 0, o1, jnp.where(tail_id == 1, o2, jnp.where(tail_id == 2, o3, 0.0))
    )
    gain_ref[6 * width :, :] = tail_rows.astype(jnp.bfloat16)

    x = xt_ref[...].T
    group = LANES // width
    x_wide = jnp.concatenate([x] * group, axis=1)
    x1, x2, x3 = (part.astype(jnp.float32) for part in split3(x_wide))
    lane = lax.broadcasted_iota(jnp.int32, (rows, LANES), 1)
    first_half = jnp.where(lane < 3 * width, x1, x2)
    second_half = jnp.where(
        lane < width, x2, jnp.where(lane < 2 * width, x3, jnp.where(lane < 2 * width + 3, 1.0, 0.0))
    )
    streamed = jnp.concatenate([first_half, second_half], axis=1).astype(jnp.bfloat16)

    quad_ref[...] = jnp.broadcast_to(start, (rows, LANES))
    tile_cols = 2 * LANES
    for t in range(cols // tile_cols):
        z = jnp.dot(
            streamed,
            gain_ref[:, t * tile_cols : (t + 1) * tile_cols],
            preferred_element_type=jnp.float32,
        )
        quad_ref[...] += z[:, :LANES] * z[:, :LANES] + z[:, LANES:] * z[:, LANES:]

    quad_t = quad_ref[...].T
    total = quad_t[:comps]
    for part in range(1, LANES // comps):
        total = total + quad_t[part * comps : (part + 1) * comps]
    log_dens = -0.5 * total
    peak = jnp.max(log_dens, axis=0, keepdims=True)
    weight = jnp.exp(log_dens - peak)
    norm = jnp.sum(weight, axis=0, keepdims=True)
    loglik = peak + jnp.log(norm)
    for line in range(rows // LANES):
        loglik_ref[line : line + 1, :] = loglik[:, line * LANES : (line + 1) * LANES]
    respons = weight / norm
    resp_parts = jnp.concatenate(split3(respons), axis=0)

    center = jnp.mean(mu, axis=1, keepdims=True)
    yt_ref[...] = xt_ref[...] - center
    total_rows = feat_ref.shape[0] // 3

    def put(base, value):
        for place, part in enumerate(split3(value)):
            at = place * total_rows + base
            feat_ref[at : at + value.shape[0], :] = part

    products = []

    def product(i, c):
        return yt_ref[i : i + 1, :] * yt_ref[c * SUB : (c + 1) * SUB, :]

    for b, c in upper_pairs(width):
        products += [product(b * SUB + i, c) for i in range(SUB)]
    sub = lax.broadcasted_iota(jnp.int32, (SUB, rows), 0)
    for b, c in diagonal_pairs(width):
        products.append(product(b * SUB, b))
        for i in range(1, SUB):
            products.append(
                jnp.where(sub >= i, product(b * SUB + i, b), product(c * SUB + i - 1, c))
            )
        products.append(product(c * SUB + SUB - 1, c))
    for at in range(0, len(products), 2):
        put(at * SUB, jnp.concatenate(products[at : at + 2], axis=0))
    _, linear, ones, _ = moment_layout(width)
    put(linear, yt_ref[...])
    put(ones, jnp.ones((total_rows - ones, rows), jnp.float32))

    sums = lax.dot_general(
        feat_ref[...],
        resp_parts,
        (((1,), (1,)), ((), ())),
        preferred_element_type=jnp.float32,
    )
    sums = sums[:total_rows] + sums[total_rows : 2 * total_rows] + sums[2 * total_rows :]
    sums = sums[:, :comps] + sums[:, comps : 2 * comps] + sums[:, 2 * comps :]
    folds = LANES // comps
    part_rows = total_rows // folds
    packed = jnp.concatenate(
        [sums[place * part_rows : (place + 1) * part_rows] for place in range(folds)], axis=1
    )
    half = mine_ref.shape[0]
    core = lax.axis_index("comp")
    lower, upper = packed[:half], packed[half:]
    mine_ref[...] = jnp.where(core == 0, lower, upper)
    other_ref[...] = jnp.where(core == 0, upper, lower)


def update(mine_ref, theirs_ref, mu, event_total):
    width, comps = mu.shape
    blocks = width // SUB
    core = lax.axis_index("comp")
    mine, theirs = mine_ref[...], theirs_ref[...]
    packed = jnp.concatenate(
        [jnp.where(core == 0, mine, theirs), jnp.where(core == 0, theirs, mine)], axis=0
    )
    sums = jnp.concatenate(
        [packed[:, place * comps : (place + 1) * comps] for place in range(LANES // comps)], axis=0
    )
    diagonal, linear, ones, _ = moment_layout(width)
    about = sums[linear : linear + width]
    counts = sums[ones : ones + 1]

    shift = mu - jnp.mean(mu, axis=1, keepdims=True)
    first = about - counts * shift
    denom = counts + prior_count
    step = first / denom
    new_mu = mu + step
    new_logw = jnp.log(denom / (event_total + comps * prior_count))

    def block(value, b):
        return value[b * SUB : (b + 1) * SUB]

    def row(value, i):
        return jnp.broadcast_to(value[i : i + 1], (SUB, comps))

    sub_id = lax.broadcasted_iota(jnp.int32, (SUB, comps), 0)
    def register(place):
        return sums[place * SUB : (place + 1) * SUB]

    raw = {}
    for place, (b, c) in enumerate(upper_pairs(width)):
        for i in range(SUB):
            raw[b * SUB + i, c] = register(place * SUB + i)
    for place, (b, c) in enumerate(diagonal_pairs(width)):
        shared = [register(diagonal // SUB + place * (SUB + 1) + i) for i in range(SUB + 1)]
        for i in range(SUB):
            raw[b * SUB + i, b] = shared[i]
            value = shared[i + 1]
            for j in range(i + 1, SUB):
                value = jnp.where(sub_id == j, row(shared[j + 1], i), value)
            raw[c * SUB + i, c] = value

    cov = [dict() for _ in range(width)]
    for (at, c), value in raw.items():
        value = value - (
            row(about, at) * block(shift, c)
            + row(shift, at) * block(first, c)
            + row(first, at) * block(step, c)
        )
        if at // SUB == c:
            value = value + jnp.where(sub_id == at % SUB, ridge, 0.0)
        cov[at][c] = value

    inverse = [
        {i // SUB: jnp.where(sub_id == i % SUB, 1.0, 0.0).astype(jnp.float32)} for i in range(width)
    ]
    factors = []
    for p in range(width):
        b = p // SUB
        pivot = cov[p][b][p % SUB : p % SUB + 1]
        recip = jnp.broadcast_to(1.0 / pivot, (SUB, comps))
        scaled = {c: cov[p][c] * recip for c in range(b, blocks)}
        for i in range(p + 1, width):
            factor = row(scaled[i // SUB], i % SUB)
            for c in range(i // SUB, blocks):
                cov[i][c] = cov[i][c] - factor * cov[p][c]
            for c in range(b + 1):
                change = factor * inverse[p][c]
                inverse[i][c] = inverse[i][c] - change if c in inverse[i] else -change
        scale = jnp.broadcast_to(jnp.sqrt(denom / pivot), (SUB, comps))
        zero = jnp.zeros((SUB, comps), jnp.float32)
        factors.append(
            jnp.concatenate(
                [inverse[p][c] * scale if c in inverse[p] else zero for c in range(blocks)], axis=0
            )
        )
    return new_mu, factors, new_logw


def place_factors(proj_ref, rows_of, comps):
    group = LANES // comps
    for t in range(len(rows_of) // group):
        proj_ref[:, t * LANES : (t + 1) * LANES] = jnp.concatenate(
            rows_of[t * group : (t + 1) * group], axis=1
        )


def first_kernel(
    xt_hbm,
    factor_hbm,
    mu_hbm,
    logw_hbm,
    loglik_ref,
    mine_ref,
    other_ref,
    xt_ref,
    sems,
    proj_ref,
    factor_ref,
    mu_ref,
    logw_ref,
    *scratch,
):
    pairs = ((factor_hbm, factor_ref), (mu_hbm, mu_ref), (logw_hbm, logw_ref), (xt_hbm, xt_ref))
    copies = [
        pltpu.make_async_copy(source, target, sems.at[place])
        for place, (source, target) in enumerate(pairs)
    ]
    for copy in copies:
        copy.start()
    for copy in copies:
        copy.wait()
    width, _, comps = factor_ref.shape
    place_factors(proj_ref, [factor_ref[i] for i in range(width)], comps)
    local_moments(
        xt_ref, proj_ref, mu_ref[...], logw_ref[...], loglik_ref, mine_ref, other_ref, *scratch
    )


def middle_kernel(
    event_total,
    xt_ref,
    mine_ref,
    theirs_ref,
    mu_ref,
    loglik_ref,
    new_mine_ref,
    new_other_ref,
    new_mu_ref,
    proj_ref,
    *scratch,
):
    mu, factors, logw = update(mine_ref, theirs_ref, mu_ref[...], event_total)
    new_mu_ref[...] = mu
    place_factors(proj_ref, factors, mu.shape[1])
    local_moments(xt_ref, proj_ref, mu, logw, loglik_ref, new_mine_ref, new_other_ref, *scratch)


def last_kernel(event_total, mine_ref, theirs_ref, mu_ref, new_mu_ref, factor_ref, logw_ref):
    mu, factors, logw = update(mine_ref, theirs_ref, mu_ref[...], event_total)
    new_mu_ref[...] = mu
    logw_ref[...] = logw
    for i, value in enumerate(factors):
        factor_ref[i] = value


def group_steps(size):
    steps, stride = [], 1
    while size > 1:
        radix = 4 if size % 4 == 0 else (2 if size % 2 == 0 else size)
        steps.append((stride, radix))
        stride *= radix
        size //= radix
    return steps


def peer(index, stride, radix, shift):
    digit = index // stride % radix
    other = digit ^ shift if radix & (radix - 1) == 0 else (digit + shift) % radix
    return index + (other - digit) * stride


def all_sum(mine, other):
    size = lax.axis_size("dp")
    swap = [(0, 1), (1, 0)]
    mine = mine + lax.ppermute(other, "comp", swap)
    for stride, radix in group_steps(size):
        order = list(range(1, radix))
        order = order[1:2] + order[:1] + order[2:] if stride == 1 else order[-1:] + order[:-1]
        received = [
            lax.ppermute(mine, "dp", [(i, peer(i, stride, radix, shift)) for i in range(size)])
            for shift in order
        ]
        for value in received:
            mine = mine + value
    return mine, lax.ppermute(mine, "comp", swap)


def body(events, means, factors, log_weights):
    rows, width = events.shape
    comps = means.shape[0]
    event_total = rows * lax.axis_size("dp") * lax.axis_size("comp")
    cols = width * comps
    f32 = jnp.float32

    total_rows = moment_layout(width)[-1]
    halves = lax.axis_size("comp")
    mom_shape = jax.ShapeDtypeStruct((total_rows * comps // LANES // halves, LANES), f32)
    loglik_shape = jax.ShapeDtypeStruct((rows // LANES, LANES), f32)
    mu_shape = jax.ShapeDtypeStruct((width, comps), f32)
    scratch = [
        pltpu.VMEM((width, cols), f32),
        pltpu.VMEM((2 * LANES, cols), jnp.bfloat16),
        pltpu.VMEM((rows, LANES), f32),
        pltpu.VMEM((3 * total_rows, rows), jnp.bfloat16),
        pltpu.VMEM((width, rows), f32),
    ]
    load = [pltpu.VMEM((width, rows), f32), pltpu.SemaphoreType.DMA((4,))]
    params = pltpu.CompilerParams(vmem_limit_bytes=24 * 1024 * 1024)
    in_hbm = pl.BlockSpec(memory_space=pltpu.HBM)

    xt = events.T
    mu = means.T
    inputs = (xt, factors.transpose(1, 2, 0), mu, log_weights.reshape(1, comps))
    loglik, mine, other = pl.pallas_call(
        first_kernel,
        out_shape=(loglik_shape, mom_shape, mom_shape),
        in_specs=[in_hbm] * 4,
        scratch_shapes=load
        + scratch[:1]
        + [
            pltpu.VMEM((width, width, comps), f32),
            pltpu.VMEM((width, comps), f32),
            pltpu.VMEM((1, comps), f32),
        ]
        + scratch[1:],
        compiler_params=params,
        name="first",
    )(*(pltpu.with_memory_space_constraint(value, pltpu.HBM) for value in inputs))
    for _ in range(1, ITERS):
        loglik, mine, other, mu = pl.pallas_call(
            functools.partial(middle_kernel, event_total),
            out_shape=(loglik_shape, mom_shape, mom_shape, mu_shape),
            scratch_shapes=scratch,
            compiler_params=params,
            name="middle",
        )(xt, *all_sum(mine, other), mu)
    mu, new_factors, logw = pl.pallas_call(
        functools.partial(last_kernel, event_total),
        out_shape=(
            mu_shape,
            jax.ShapeDtypeStruct((width, width, comps), f32),
            jax.ShapeDtypeStruct((1, comps), f32),
        ),
        compiler_params=params,
        name="last",
    )(*all_sum(mine, other), mu)
    return mu.T, new_factors.transpose(2, 0, 1), logw.reshape(comps), loglik.reshape(rows)


def solution(mesh):
    in_specs = (P(("dp", "comp"), None), P(), P(), P())
    out_specs = (P(), P(), P(), P(("dp", "comp")))
    return jax.shard_map(body, mesh=mesh, in_specs=in_specs, out_specs=out_specs, check_vma=False)
```

```python
import functools
import math

import jax
import jax.numpy as jnp
from jax import lax
from jax.experimental import pallas as pl
from jax.experimental.pallas import tpu as pltpu
from jax.sharding import PartitionSpec as P

ITERS = 2
SUB = 8
LANES = 128
MASKS = (0, 1)

ridge = 0.1
prior_count = 1.0


def split3(value):
    high = value.astype(jnp.bfloat16)
    rest = value - high.astype(jnp.float32)
    mid = rest.astype(jnp.bfloat16)
    low = (rest - mid.astype(jnp.float32)).astype(jnp.bfloat16)
    return high, mid, low


def upper_pairs(width):
    blocks = width // SUB
    return [(b, c) for b in range(blocks) for c in range(b + 1, blocks)]


def diagonal_pairs(width):
    return [(b, b + 1) for b in range(0, width // SUB, 2)]


def moment_layout(width):
    diagonal = len(upper_pairs(width)) * SUB * SUB
    linear = diagonal + len(diagonal_pairs(width)) * SUB * (SUB + 1)
    ones = linear + width
    step = 4 * SUB * 2
    return diagonal, linear, ones, -(-(ones + 1) // step) * step


def local_moments(
    xt_ref, proj_ref, mu, logw, loglik_ref, mine_ref, other_ref, gain_ref, quad_ref, feat_ref, yt_ref
):
    width, rows = xt_ref.shape
    comps = mu.shape[1]
    cols = width * comps
    proj = proj_ref[...]
    reps = cols // LANES

    mu_wide = jnp.concatenate([mu] * (LANES // comps), axis=1)
    sub_id = lax.broadcasted_iota(jnp.int32, (width, LANES), 0)
    lane_id = lax.broadcasted_iota(jnp.int32, (width, LANES), 1) // comps
    log_det = jnp.zeros((1, LANES), jnp.float32)
    offsets = []
    for t in range(reps):
        tile = proj[:, t * LANES : (t + 1) * LANES]
        offsets.append(jnp.sum(tile * mu_wide, axis=0, keepdims=True))
        row_of = lane_id + t * (LANES // comps)
        diag = jnp.sum(jnp.where(sub_id == row_of, tile, 0.0), axis=0, keepdims=True)
        log_det = log_det + jnp.log(diag)
    offset = jnp.concatenate(offsets, axis=1)

    logw_max = jnp.max(logw, axis=1, keepdims=True)
    logw_lse = logw_max + jnp.log(jnp.sum(jnp.exp(logw - logw_max), axis=1, keepdims=True))
    constant = logw - logw_lse - 0.5 * width * math.log(2.0 * math.pi)
    start = -2.0 * (
        log_det + jnp.concatenate([constant] + [jnp.zeros_like(constant)] * (LANES // comps - 1), axis=1)
    )

    p1, p2, p3 = split3(proj)
    for place, part in enumerate((p1, p2, p3, p1, p2, p1)):
        gain_ref[place * width : (place + 1) * width, :] = part
    depth = gain_ref.shape[0]
    tail = depth - 6 * width
    o1, o2, o3 = (part.astype(jnp.float32) for part in split3(-offset))
    tail_id = lax.broadcasted_iota(jnp.int32, (tail, cols), 0)
    tail_rows = jnp.where(
        tail_id == 0, o1, jnp.where(tail_id == 1, o2, jnp.where(tail_id == 2, o3, 0.0))
    )
    gain_ref[6 * width :, :] = tail_rows.astype(jnp.bfloat16)

    x = xt_ref[...].T
    group = LANES // width
    x_wide = jnp.concatenate([x] * group, axis=1)
    x1, x2, x3 = (part.astype(jnp.float32) for part in split3(x_wide))
    lane = lax.broadcasted_iota(jnp.int32, (rows, LANES), 1)
    first_half = jnp.where(lane < 3 * width, x1, x2)
    second_half = jnp.where(
        lane < width, x2, jnp.where(lane < 2 * width, x3, jnp.where(lane < 2 * width + 3, 1.0, 0.0))
    )
    streamed = jnp.concatenate([first_half, second_half], axis=1).astype(jnp.bfloat16)

    quad_ref[...] = jnp.broadcast_to(start, (rows, LANES))
    tile_cols = 2 * LANES
    for t in range(cols // tile_cols):
        z = jnp.dot(
            streamed,
            gain_ref[:, t * tile_cols : (t + 1) * tile_cols],
            preferred_element_type=jnp.float32,
        )
        quad_ref[...] += z[:, :LANES] * z[:, :LANES] + z[:, LANES:] * z[:, LANES:]

    quad_t = quad_ref[...].T
    total = quad_t[:comps]
    for part in range(1, LANES // comps):
        total = total + quad_t[part * comps : (part + 1) * comps]
    log_dens = -0.5 * total
    peak = jnp.max(log_dens, axis=0, keepdims=True)
    weight = jnp.exp(log_dens - peak)
    norm = jnp.sum(weight, axis=0, keepdims=True)
    loglik = peak + jnp.log(norm)
    for line in range(rows // LANES):
        loglik_ref[line : line + 1, :] = loglik[:, line * LANES : (line + 1) * LANES]
    respons = weight / norm
    resp_parts = jnp.concatenate(split3(respons), axis=0)

    center = jnp.mean(mu, axis=1, keepdims=True)
    yt_ref[...] = xt_ref[...] - center
    total_rows = feat_ref.shape[0] // 3

    def put(base, value):
        for place, part in enumerate(split3(value)):
            at = place * total_rows + base
            feat_ref[at : at + value.shape[0], :] = part

    products = []

    def product(i, c):
        return yt_ref[i : i + 1, :] * yt_ref[c * SUB : (c + 1) * SUB, :]

    for b, c in upper_pairs(width):
        products += [product(b * SUB + i, c) for i in range(SUB)]
    sub = lax.broadcasted_iota(jnp.int32, (SUB, rows), 0)
    for b, c in diagonal_pairs(width):
        products.append(product(b * SUB, b))
        for i in range(1, SUB):
            products.append(
                jnp.where(sub >= i, product(b * SUB + i, b), product(c * SUB + i - 1, c))
            )
        products.append(product(c * SUB + SUB - 1, c))
    for at in range(0, len(products), 2):
        put(at * SUB, jnp.concatenate(products[at : at + 2], axis=0))
    _, linear, ones, _ = moment_layout(width)
    put(linear, yt_ref[...])
    put(ones, jnp.ones((total_rows - ones, rows), jnp.float32))

    sums = lax.dot_general(
        feat_ref[...],
        resp_parts,
        (((1,), (1,)), ((), ())),
        preferred_element_type=jnp.float32,
    )
    sums = sums[:total_rows] + sums[total_rows : 2 * total_rows] + sums[2 * total_rows :]
    sums = sums[:, :comps] + sums[:, comps : 2 * comps] + sums[:, 2 * comps :]
    folds = LANES // comps
    part_rows = total_rows // folds
    packed = jnp.concatenate(
        [sums[place * part_rows : (place + 1) * part_rows] for place in range(folds)], axis=1
    )
    half = mine_ref.shape[0]
    core = own_half()
    lower, upper = packed[:half], packed[half:]
    mine_ref[...] = jnp.where(core == 0, lower, upper)
    other_ref[...] = jnp.where(core == 0, upper, lower)


def update(mine_ref, theirs_ref, mu, event_total):
    width, comps = mu.shape
    blocks = width // SUB
    core = own_half()
    mine, theirs = mine_ref[...], theirs_ref[...]
    packed = jnp.concatenate(
        [jnp.where(core == 0, mine, theirs), jnp.where(core == 0, theirs, mine)], axis=0
    )
    sums = jnp.concatenate(
        [packed[:, place * comps : (place + 1) * comps] for place in range(LANES // comps)], axis=0
    )
    diagonal, linear, ones, _ = moment_layout(width)
    about = sums[linear : linear + width]
    counts = sums[ones : ones + 1]

    shift = mu - jnp.mean(mu, axis=1, keepdims=True)
    first = about - counts * shift
    denom = counts + prior_count
    step = first / denom
    new_mu = mu + step
    new_logw = jnp.log(denom / (event_total + comps * prior_count))

    def block(value, b):
        return value[b * SUB : (b + 1) * SUB]

    def row(value, i):
        return jnp.broadcast_to(value[i : i + 1], (SUB, comps))

    sub_id = lax.broadcasted_iota(jnp.int32, (SUB, comps), 0)
    def register(place):
        return sums[place * SUB : (place + 1) * SUB]

    raw = {}
    for place, (b, c) in enumerate(upper_pairs(width)):
        for i in range(SUB):
            raw[b * SUB + i, c] = register(place * SUB + i)
    for place, (b, c) in enumerate(diagonal_pairs(width)):
        shared = [register(diagonal // SUB + place * (SUB + 1) + i) for i in range(SUB + 1)]
        for i in range(SUB):
            raw[b * SUB + i, b] = shared[i]
            value = shared[i + 1]
            for j in range(i + 1, SUB):
                value = jnp.where(sub_id == j, row(shared[j + 1], i), value)
            raw[c * SUB + i, c] = value

    cov = [dict() for _ in range(width)]
    for (at, c), value in raw.items():
        value = value - (
            row(about, at) * block(shift, c)
            + row(shift, at) * block(first, c)
            + row(first, at) * block(step, c)
        )
        if at // SUB == c:
            value = value + jnp.where(sub_id == at % SUB, ridge, 0.0)
        cov[at][c] = value

    inverse = [
        {i // SUB: jnp.where(sub_id == i % SUB, 1.0, 0.0).astype(jnp.float32)} for i in range(width)
    ]
    factors = []
    for p in range(width):
        b = p // SUB
        pivot = cov[p][b][p % SUB : p % SUB + 1]
        recip = jnp.broadcast_to(1.0 / pivot, (SUB, comps))
        scaled = {c: cov[p][c] * recip for c in range(b, blocks)}
        for i in range(p + 1, width):
            factor = row(scaled[i // SUB], i % SUB)
            for c in range(i // SUB, blocks):
                cov[i][c] = cov[i][c] - factor * cov[p][c]
            for c in range(b + 1):
                change = factor * inverse[p][c]
                inverse[i][c] = inverse[i][c] - change if c in inverse[i] else -change
        scale = jnp.broadcast_to(jnp.sqrt(denom / pivot), (SUB, comps))
        zero = jnp.zeros((SUB, comps), jnp.float32)
        factors.append(
            jnp.concatenate(
                [inverse[p][c] * scale if c in inverse[p] else zero for c in range(blocks)], axis=0
            )
        )
    return new_mu, factors, new_logw


def place_factors(proj_ref, rows_of, comps):
    group = LANES // comps
    for t in range(len(rows_of) // group):
        proj_ref[:, t * LANES : (t + 1) * LANES] = jnp.concatenate(
            rows_of[t * group : (t + 1) * group], axis=1
        )


def first_kernel(
    xt_hbm,
    factor_hbm,
    mu_hbm,
    logw_hbm,
    loglik_ref,
    mine_ref,
    other_ref,
    xt_ref,
    sems,
    proj_ref,
    factor_ref,
    mu_ref,
    logw_ref,
    *scratch,
):
    pairs = ((factor_hbm, factor_ref), (mu_hbm, mu_ref), (logw_hbm, logw_ref), (xt_hbm, xt_ref))
    copies = [
        pltpu.make_async_copy(source, target, sems.at[place])
        for place, (source, target) in enumerate(pairs)
    ]
    for copy in copies:
        copy.start()
    for copy in copies:
        copy.wait()
    width, _, comps = factor_ref.shape
    place_factors(proj_ref, [factor_ref[i] for i in range(width)], comps)
    local_moments(
        xt_ref, proj_ref, mu_ref[...], logw_ref[...], loglik_ref, mine_ref, other_ref, *scratch
    )


def middle_kernel(
    event_total,
    xt_ref,
    mine_ref,
    theirs_ref,
    mu_ref,
    loglik_ref,
    new_mine_ref,
    new_other_ref,
    new_mu_ref,
    proj_ref,
    *scratch,
):
    mu, factors, logw = update(mine_ref, theirs_ref, mu_ref[...], event_total)
    new_mu_ref[...] = mu
    place_factors(proj_ref, factors, mu.shape[1])
    local_moments(xt_ref, proj_ref, mu, logw, loglik_ref, new_mine_ref, new_other_ref, *scratch)


def last_kernel(event_total, mine_ref, theirs_ref, mu_ref, new_mu_ref, factor_ref, logw_ref):
    mu, factors, logw = update(mine_ref, theirs_ref, mu_ref[...], event_total)
    new_mu_ref[...] = mu
    logw_ref[...] = logw
    for i, value in enumerate(factors):
        factor_ref[i] = value


def group_steps(size):
    steps, stride = [], 1
    while size > 1:
        radix = 4 if size % 4 == 0 else (2 if size % 2 == 0 else size)
        steps.append((stride, radix))
        stride *= radix
        size //= radix
    return steps


def peer(index, stride, radix, shift):
    digit = index // stride % radix
    other = digit ^ shift if radix & (radix - 1) == 0 else (digit + shift) % radix
    return index + (other - digit) * stride


def own_half():
    owner = lax.axis_index("comp")
    chip = lax.axis_index("dp")
    for stride, radix in group_steps(lax.axis_size("dp")):
        mask = crossing_mask(stride, radix)
        digit = chip // stride % radix
        for bit in (1, 2):
            if mask & bit:
                owner = owner + digit // bit % 2
    return owner % 2


def crossing_mask(stride, radix):
    if radix != 4:
        return 0
    return MASKS[0] if stride == 1 else MASKS[1]


def all_sum(mine, other):
    size = lax.axis_size("dp")
    cores = lax.axis_size("comp")
    swap = [(0, 1), (1, 0)]
    mine = mine + lax.ppermute(other, "comp", swap)
    for stride, radix in group_steps(size):
        order = list(range(1, radix))
        order = order[1:2] + order[:1] + order[2:] if stride == 1 else order[::2] + order[1::2]
        received = []
        for shift in order:
            flip = bin(shift & crossing_mask(stride, radix)).count("1") % 2
            pairs = [
                (i * cores + c, peer(i, stride, radix, shift) * cores + (c ^ flip))
                for i in range(size)
                for c in range(cores)
            ]
            received.append(lax.ppermute(mine, ("dp", "comp"), pairs))
        for value in received:
            mine = mine + value
    return mine, lax.ppermute(mine, "comp", swap)


def body(events, means, factors, log_weights):
    rows, width = events.shape
    comps = means.shape[0]
    event_total = rows * lax.axis_size("dp") * lax.axis_size("comp")
    cols = width * comps
    f32 = jnp.float32

    total_rows = moment_layout(width)[-1]
    halves = lax.axis_size("comp")
    mom_shape = jax.ShapeDtypeStruct((total_rows * comps // LANES // halves, LANES), f32)
    loglik_shape = jax.ShapeDtypeStruct((rows // LANES, LANES), f32)
    mu_shape = jax.ShapeDtypeStruct((width, comps), f32)
    scratch = [
        pltpu.VMEM((width, cols), f32),
        pltpu.VMEM((2 * LANES, cols), jnp.bfloat16),
        pltpu.VMEM((rows, LANES), f32),
        pltpu.VMEM((3 * total_rows, rows), jnp.bfloat16),
        pltpu.VMEM((width, rows), f32),
    ]
    load = [pltpu.VMEM((width, rows), f32), pltpu.SemaphoreType.DMA((4,))]
    params = pltpu.CompilerParams(vmem_limit_bytes=24 * 1024 * 1024)
    in_hbm = pl.BlockSpec(memory_space=pltpu.HBM)

    xt = events.T
    mu = means.T
    inputs = (xt, factors.transpose(1, 2, 0), mu, log_weights.reshape(1, comps))
    loglik, mine, other = pl.pallas_call(
        first_kernel,
        out_shape=(loglik_shape, mom_shape, mom_shape),
        in_specs=[in_hbm] * 4,
        scratch_shapes=load
        + scratch[:1]
        + [
            pltpu.VMEM((width, width, comps), f32),
            pltpu.VMEM((width, comps), f32),
            pltpu.VMEM((1, comps), f32),
        ]
        + scratch[1:],
        compiler_params=params,
        name="first",
    )(*(pltpu.with_memory_space_constraint(value, pltpu.HBM) for value in inputs))
    for _ in range(1, ITERS):
        loglik, mine, other, mu = pl.pallas_call(
            functools.partial(middle_kernel, event_total),
            out_shape=(loglik_shape, mom_shape, mom_shape, mu_shape),
            scratch_shapes=scratch,
            compiler_params=params,
            name="middle",
        )(xt, *all_sum(mine, other), mu)
    mu, new_factors, logw = pl.pallas_call(
        functools.partial(last_kernel, event_total),
        out_shape=(
            mu_shape,
            jax.ShapeDtypeStruct((width, width, comps), f32),
            jax.ShapeDtypeStruct((1, comps), f32),
        ),
        compiler_params=params,
        name="last",
    )(*all_sum(mine, other), mu)
    return mu.T, new_factors.transpose(2, 0, 1), logw.reshape(comps), loglik.reshape(rows)


def solution(mesh):
    in_specs = (P(("dp", "comp"), None), P(), P(), P())
    out_specs = (P(), P(), P(), P(("dp", "comp")))
    return jax.shard_map(body, mesh=mesh, in_specs=in_specs, out_specs=out_specs, check_vma=False)
```

```python
import functools
import math

import jax
import jax.numpy as jnp
from jax import lax
from jax.experimental import pallas as pl
from jax.experimental.pallas import tpu as pltpu
from jax.sharding import PartitionSpec as P

ITERS = 2
SUB = 8
LANES = 128
MASKS = (0, 1)

ridge = 0.1
prior_count = 1.0


def split3(value):
    high = value.astype(jnp.bfloat16)
    rest = value - high.astype(jnp.float32)
    mid = rest.astype(jnp.bfloat16)
    low = (rest - mid.astype(jnp.float32)).astype(jnp.bfloat16)
    return high, mid, low


def upper_pairs(width):
    blocks = width // SUB
    return [(b, c) for b in range(blocks) for c in range(b + 1, blocks)]


def diagonal_pairs(width):
    return [(b, b + 1) for b in range(0, width // SUB, 2)]


def moment_layout(width):
    diagonal = len(upper_pairs(width)) * SUB * SUB
    linear = diagonal + len(diagonal_pairs(width)) * SUB * (SUB + 1)
    ones = linear + width
    step = 4 * SUB * 2
    return diagonal, linear, ones, -(-(ones + 1) // step) * step


def local_moments(
    xt_ref, proj_ref, mu, logw, loglik_ref, mine_ref, other_ref, gain_ref, quad_ref, feat_ref, yt_ref
):
    width, rows = xt_ref.shape
    comps = mu.shape[1]
    cols = width * comps
    proj = proj_ref[...]
    reps = cols // LANES

    mu_wide = jnp.concatenate([mu] * (LANES // comps), axis=1)
    sub_id = lax.broadcasted_iota(jnp.int32, (width, LANES), 0)
    lane_id = lax.broadcasted_iota(jnp.int32, (width, LANES), 1) // comps
    log_det = jnp.zeros((1, LANES), jnp.float32)
    offsets = []
    for t in range(reps):
        tile = proj[:, t * LANES : (t + 1) * LANES]
        offsets.append(jnp.sum(tile * mu_wide, axis=0, keepdims=True))
        row_of = lane_id + t * (LANES // comps)
        diag = jnp.sum(jnp.where(sub_id == row_of, tile, 0.0), axis=0, keepdims=True)
        log_det = log_det + jnp.log(diag)
    offset = jnp.concatenate(offsets, axis=1)

    logw_max = jnp.max(logw, axis=1, keepdims=True)
    logw_lse = logw_max + jnp.log(jnp.sum(jnp.exp(logw - logw_max), axis=1, keepdims=True))
    constant = logw - logw_lse - 0.5 * width * math.log(2.0 * math.pi)
    start = -2.0 * (
        log_det + jnp.concatenate([constant] + [jnp.zeros_like(constant)] * (LANES // comps - 1), axis=1)
    )

    p1, p2, p3 = split3(proj)
    for place, part in enumerate((p1, p2, p3, p1, p2, p1)):
        gain_ref[place * width : (place + 1) * width, :] = part
    depth = gain_ref.shape[0]
    tail = depth - 6 * width
    o1, o2, o3 = (part.astype(jnp.float32) for part in split3(-offset))
    tail_id = lax.broadcasted_iota(jnp.int32, (tail, cols), 0)
    tail_rows = jnp.where(
        tail_id == 0, o1, jnp.where(tail_id == 1, o2, jnp.where(tail_id == 2, o3, 0.0))
    )
    gain_ref[6 * width :, :] = tail_rows.astype(jnp.bfloat16)

    x = xt_ref[...].T
    group = LANES // width
    x_wide = jnp.concatenate([x] * group, axis=1)
    x1, x2, x3 = (part.astype(jnp.float32) for part in split3(x_wide))
    lane = lax.broadcasted_iota(jnp.int32, (rows, LANES), 1)
    first_half = jnp.where(lane < 3 * width, x1, x2)
    second_half = jnp.where(
        lane < width, x2, jnp.where(lane < 2 * width, x3, jnp.where(lane < 2 * width + 3, 1.0, 0.0))
    )
    streamed = jnp.concatenate([first_half, second_half], axis=1).astype(jnp.bfloat16)

    quad_ref[...] = jnp.broadcast_to(start, (rows, LANES))
    tile_cols = 2 * LANES
    for t in range(cols // tile_cols):
        z = jnp.dot(
            streamed,
            gain_ref[:, t * tile_cols : (t + 1) * tile_cols],
            preferred_element_type=jnp.float32,
        )
        quad_ref[...] += z[:, :LANES] * z[:, :LANES] + z[:, LANES:] * z[:, LANES:]

    quad_t = quad_ref[...].T
    total = quad_t[:comps]
    for part in range(1, LANES // comps):
        total = total + quad_t[part * comps : (part + 1) * comps]
    log_dens = -0.5 * total
    peak = jnp.max(log_dens, axis=0, keepdims=True)
    weight = jnp.exp(log_dens - peak)
    norm = jnp.sum(weight, axis=0, keepdims=True)
    loglik = peak + jnp.log(norm)
    if loglik_ref is not None:
        for line in range(rows // LANES):
            loglik_ref[line : line + 1, :] = loglik[:, line * LANES : (line + 1) * LANES]
    respons = weight / norm
    resp_parts = jnp.concatenate(split3(respons), axis=0)

    center = jnp.mean(mu, axis=1, keepdims=True)
    yt_ref[...] = xt_ref[...] - center
    total_rows = feat_ref.shape[0] // 3

    def put(base, value):
        for place, part in enumerate(split3(value)):
            at = place * total_rows + base
            feat_ref[at : at + value.shape[0], :] = part

    products = []

    def product(i, c):
        return yt_ref[i : i + 1, :] * yt_ref[c * SUB : (c + 1) * SUB, :]

    for b, c in upper_pairs(width):
        products += [product(b * SUB + i, c) for i in range(SUB)]
    sub = lax.broadcasted_iota(jnp.int32, (SUB, rows), 0)
    for b, c in diagonal_pairs(width):
        products.append(product(b * SUB, b))
        for i in range(1, SUB):
            products.append(
                jnp.where(sub >= i, product(b * SUB + i, b), product(c * SUB + i - 1, c))
            )
        products.append(product(c * SUB + SUB - 1, c))
    for at in range(0, len(products), 2):
        put(at * SUB, jnp.concatenate(products[at : at + 2], axis=0))
    _, linear, ones, _ = moment_layout(width)
    put(linear, yt_ref[...])
    put(ones, jnp.ones((total_rows - ones, rows), jnp.float32))

    sums = lax.dot_general(
        feat_ref[...],
        resp_parts,
        (((1,), (1,)), ((), ())),
        preferred_element_type=jnp.float32,
    )
    sums = sums[:total_rows] + sums[total_rows : 2 * total_rows] + sums[2 * total_rows :]
    sums = sums[:, :comps] + sums[:, comps : 2 * comps] + sums[:, 2 * comps :]
    folds = LANES // comps
    part_rows = total_rows // folds
    packed = jnp.concatenate(
        [sums[place * part_rows : (place + 1) * part_rows] for place in range(folds)], axis=1
    )
    half = mine_ref.shape[0]
    core = own_half()
    lower, upper = packed[:half], packed[half:]
    mine_ref[...] = jnp.where(core == 0, lower, upper)
    other_ref[...] = jnp.where(core == 0, upper, lower)


def update(mine_ref, theirs_ref, mu, event_total):
    width, comps = mu.shape
    blocks = width // SUB
    core = own_half()
    mine, theirs = mine_ref[...], theirs_ref[...]
    packed = jnp.concatenate(
        [jnp.where(core == 0, mine, theirs), jnp.where(core == 0, theirs, mine)], axis=0
    )
    sums = jnp.concatenate(
        [packed[:, place * comps : (place + 1) * comps] for place in range(LANES // comps)], axis=0
    )
    diagonal, linear, ones, _ = moment_layout(width)
    about = sums[linear : linear + width]
    counts = sums[ones : ones + 1]

    shift = mu - jnp.mean(mu, axis=1, keepdims=True)
    first = about - counts * shift
    denom = counts + prior_count
    step = first / denom
    new_mu = mu + step
    new_logw = jnp.log(denom / (event_total + comps * prior_count))

    def block(value, b):
        return value[b * SUB : (b + 1) * SUB]

    def row(value, i):
        return jnp.broadcast_to(value[i : i + 1], (SUB, comps))

    sub_id = lax.broadcasted_iota(jnp.int32, (SUB, comps), 0)
    def register(place):
        return sums[place * SUB : (place + 1) * SUB]

    raw = {}
    for place, (b, c) in enumerate(upper_pairs(width)):
        for i in range(SUB):
            raw[b * SUB + i, c] = register(place * SUB + i)
    for place, (b, c) in enumerate(diagonal_pairs(width)):
        shared = [register(diagonal // SUB + place * (SUB + 1) + i) for i in range(SUB + 1)]
        for i in range(SUB):
            raw[b * SUB + i, b] = shared[i]
            value = shared[i + 1]
            for j in range(i + 1, SUB):
                value = jnp.where(sub_id == j, row(shared[j + 1], i), value)
            raw[c * SUB + i, c] = value

    cov = [dict() for _ in range(width)]
    for (at, c), value in raw.items():
        value = value - (
            row(about, at) * block(shift, c)
            + row(shift, at) * block(first, c)
            + row(first, at) * block(step, c)
        )
        if at // SUB == c:
            value = value + jnp.where(sub_id == at % SUB, ridge, 0.0)
        cov[at][c] = value

    inverse = [
        {i // SUB: jnp.where(sub_id == i % SUB, 1.0, 0.0).astype(jnp.float32)} for i in range(width)
    ]
    factors = []
    for p in range(width):
        b = p // SUB
        pivot = cov[p][b][p % SUB : p % SUB + 1]
        recip = jnp.broadcast_to(1.0 / pivot, (SUB, comps))
        scaled = {c: cov[p][c] * recip for c in range(b, blocks)}
        for i in range(p + 1, width):
            factor = row(scaled[i // SUB], i % SUB)
            for c in range(i // SUB, blocks):
                cov[i][c] = cov[i][c] - factor * cov[p][c]
            for c in range(b + 1):
                change = factor * inverse[p][c]
                inverse[i][c] = inverse[i][c] - change if c in inverse[i] else -change
        scale = jnp.broadcast_to(jnp.sqrt(denom / pivot), (SUB, comps))
        zero = jnp.zeros((SUB, comps), jnp.float32)
        factors.append(
            jnp.concatenate(
                [inverse[p][c] * scale if c in inverse[p] else zero for c in range(blocks)], axis=0
            )
        )
    return new_mu, factors, new_logw


def place_factors(proj_ref, rows_of, comps):
    group = LANES // comps
    for t in range(len(rows_of) // group):
        proj_ref[:, t * LANES : (t + 1) * LANES] = jnp.concatenate(
            rows_of[t * group : (t + 1) * group], axis=1
        )


def first_kernel(
    xt_hbm,
    factor_hbm,
    mu_hbm,
    logw_hbm,
    mine_ref,
    other_ref,
    xt_ref,
    sems,
    proj_ref,
    factor_ref,
    mu_ref,
    logw_ref,
    *scratch,
):
    pairs = ((factor_hbm, factor_ref), (mu_hbm, mu_ref), (logw_hbm, logw_ref), (xt_hbm, xt_ref))
    copies = [
        pltpu.make_async_copy(source, target, sems.at[place])
        for place, (source, target) in enumerate(pairs)
    ]
    for copy in copies:
        copy.start()
    for copy in copies:
        copy.wait()
    width, _, comps = factor_ref.shape
    place_factors(proj_ref, [factor_ref[i] for i in range(width)], comps)
    local_moments(
        xt_ref, proj_ref, mu_ref[...], logw_ref[...], None, mine_ref, other_ref, *scratch
    )


def middle_kernel(
    event_total,
    xt_ref,
    mine_ref,
    theirs_ref,
    mu_ref,
    loglik_ref,
    new_mine_ref,
    new_other_ref,
    new_mu_ref,
    proj_ref,
    *scratch,
):
    mu, factors, logw = update(mine_ref, theirs_ref, mu_ref[...], event_total)
    new_mu_ref[...] = mu
    place_factors(proj_ref, factors, mu.shape[1])
    local_moments(xt_ref, proj_ref, mu, logw, loglik_ref, new_mine_ref, new_other_ref, *scratch)


def last_kernel(
    event_total,
    mine_ref,
    theirs_ref,
    mu_ref,
    loglik_ref,
    new_mu_ref,
    factor_ref,
    logw_ref,
    loglik_out_ref,
):
    loglik_out_ref[...] = loglik_ref[...]
    mu, factors, logw = update(mine_ref, theirs_ref, mu_ref[...], event_total)
    new_mu_ref[...] = mu
    logw_ref[...] = logw
    for i, value in enumerate(factors):
        factor_ref[i] = value


def group_steps(size):
    steps, stride = [], 1
    while size > 1:
        radix = 4 if size % 4 == 0 else (2 if size % 2 == 0 else size)
        steps.append((stride, radix))
        stride *= radix
        size //= radix
    return steps


def peer(index, stride, radix, shift):
    digit = index // stride % radix
    other = digit ^ shift if radix & (radix - 1) == 0 else (digit + shift) % radix
    return index + (other - digit) * stride


def own_half():
    owner = lax.axis_index("comp")
    chip = lax.axis_index("dp")
    for stride, radix in group_steps(lax.axis_size("dp")):
        mask = crossing_mask(stride, radix)
        digit = chip // stride % radix
        for bit in (1, 2):
            if mask & bit:
                owner = owner + digit // bit % 2
    return owner % 2


def crossing_mask(stride, radix):
    if radix != 4:
        return 0
    return MASKS[0] if stride == 1 else MASKS[1]


def all_sum(mine, other):
    size = lax.axis_size("dp")
    cores = lax.axis_size("comp")
    swap = [(0, 1), (1, 0)]
    mine = mine + lax.ppermute(other, "comp", swap)
    for stride, radix in group_steps(size):
        order = list(range(1, radix))
        order = order[1:2] + order[:1] + order[2:] if stride == 1 else order[::2] + order[1::2]
        received = []
        for shift in order:
            flip = bin(shift & crossing_mask(stride, radix)).count("1") % 2
            pairs = [
                (i * cores + c, peer(i, stride, radix, shift) * cores + (c ^ flip))
                for i in range(size)
                for c in range(cores)
            ]
            received.append(lax.ppermute(mine, ("dp", "comp"), pairs))
        for value in received:
            mine = mine + value
    return mine, lax.ppermute(mine, "comp", swap)


def body(events, means, factors, log_weights):
    rows, width = events.shape
    comps = means.shape[0]
    event_total = rows * lax.axis_size("dp") * lax.axis_size("comp")
    cols = width * comps
    f32 = jnp.float32

    total_rows = moment_layout(width)[-1]
    halves = lax.axis_size("comp")
    mom_shape = jax.ShapeDtypeStruct((total_rows * comps // LANES // halves, LANES), f32)
    loglik_shape = jax.ShapeDtypeStruct((rows // LANES, LANES), f32)
    mu_shape = jax.ShapeDtypeStruct((width, comps), f32)
    scratch = [
        pltpu.VMEM((width, cols), f32),
        pltpu.VMEM((2 * LANES, cols), jnp.bfloat16),
        pltpu.VMEM((rows, LANES), f32),
        pltpu.VMEM((3 * total_rows, rows), jnp.bfloat16),
        pltpu.VMEM((width, rows), f32),
    ]
    load = [pltpu.VMEM((width, rows), f32), pltpu.SemaphoreType.DMA((4,))]
    params = pltpu.CompilerParams(vmem_limit_bytes=24 * 1024 * 1024)
    in_hbm = pl.BlockSpec(memory_space=pltpu.HBM)

    xt = events.T
    mu = means.T
    inputs = (xt, factors.transpose(1, 2, 0), mu, log_weights.reshape(1, comps))
    mine, other = pl.pallas_call(
        first_kernel,
        out_shape=(mom_shape, mom_shape),
        in_specs=[in_hbm] * 4,
        scratch_shapes=load
        + scratch[:1]
        + [
            pltpu.VMEM((width, width, comps), f32),
            pltpu.VMEM((width, comps), f32),
            pltpu.VMEM((1, comps), f32),
        ]
        + scratch[1:],
        compiler_params=params,
        name="first",
    )(*(pltpu.with_memory_space_constraint(value, pltpu.HBM) for value in inputs))
    for _ in range(1, ITERS):
        loglik, mine, other, mu = pl.pallas_call(
            functools.partial(middle_kernel, event_total),
            out_shape=(loglik_shape, mom_shape, mom_shape, mu_shape),
            scratch_shapes=scratch,
            compiler_params=params,
            name="middle",
        )(xt, *all_sum(mine, other), mu)
    mu, new_factors, logw, loglik = pl.pallas_call(
        functools.partial(last_kernel, event_total),
        out_shape=(
            mu_shape,
            jax.ShapeDtypeStruct((width, width, comps), f32),
            jax.ShapeDtypeStruct((1, comps), f32),
            loglik_shape,
        ),
        compiler_params=params,
        name="last",
    )(*all_sum(mine, other), mu, loglik)
    return mu.T, new_factors.transpose(2, 0, 1), logw.reshape(comps), loglik.reshape(rows)


def solution(mesh):
    in_specs = (P(("dp", "comp"), None), P(), P(), P())
    out_specs = (P(), P(), P(), P(("dp", "comp")))
    return jax.shard_map(body, mesh=mesh, in_specs=in_specs, out_specs=out_specs, check_vma=False)
```

```python
import functools
import math

import jax
import jax.numpy as jnp
from jax import lax
from jax.experimental import pallas as pl
from jax.experimental.pallas import tpu as pltpu
from jax.sharding import PartitionSpec as P

ITERS = 2
SUB = 8
LANES = 128
MASKS = (0, 1)

ridge = 0.1
prior_count = 1.0


def split3(value):
    high = value.astype(jnp.bfloat16)
    rest = value - high.astype(jnp.float32)
    mid = rest.astype(jnp.bfloat16)
    low = (rest - mid.astype(jnp.float32)).astype(jnp.bfloat16)
    return high, mid, low


def upper_pairs(width):
    blocks = width // SUB
    return [(b, c) for b in range(blocks) for c in range(b + 1, blocks)]


def diagonal_pairs(width):
    return [(b, b + 1) for b in range(0, width // SUB, 2)]


def moment_layout(width):
    diagonal = len(upper_pairs(width)) * SUB * SUB
    linear = diagonal + len(diagonal_pairs(width)) * SUB * (SUB + 1)
    ones = linear + width
    step = 4 * SUB * 2
    return diagonal, linear, ones, -(-(ones + 1) // step) * step


def local_moments(
    xt_ref, proj_ref, mu, logw, loglik_ref, mine_ref, other_ref, gain_ref, quad_ref, feat_ref, yt_ref
):
    width, rows = xt_ref.shape
    comps = mu.shape[1]
    cols = width * comps
    proj = proj_ref[...]
    reps = cols // LANES

    mu_wide = jnp.concatenate([mu] * (LANES // comps), axis=1)
    sub_id = lax.broadcasted_iota(jnp.int32, (width, LANES), 0)
    lane_id = lax.broadcasted_iota(jnp.int32, (width, LANES), 1) // comps
    log_det = jnp.zeros((1, LANES), jnp.float32)
    offsets = []
    for t in range(reps):
        tile = proj[:, t * LANES : (t + 1) * LANES]
        offsets.append(jnp.sum(tile * mu_wide, axis=0, keepdims=True))
        row_of = lane_id + t * (LANES // comps)
        diag = jnp.sum(jnp.where(sub_id == row_of, tile, 0.0), axis=0, keepdims=True)
        log_det = log_det + jnp.log(diag)
    offset = jnp.concatenate(offsets, axis=1)

    logw_max = jnp.max(logw, axis=1, keepdims=True)
    logw_lse = logw_max + jnp.log(jnp.sum(jnp.exp(logw - logw_max), axis=1, keepdims=True))
    constant = logw - logw_lse - 0.5 * width * math.log(2.0 * math.pi)
    start = -2.0 * (
        log_det + jnp.concatenate([constant] + [jnp.zeros_like(constant)] * (LANES // comps - 1), axis=1)
    )

    p1, p2, p3 = split3(proj)
    for place, part in enumerate((p1, p2, p3, p1, p2, p1)):
        gain_ref[place * width : (place + 1) * width, :] = part
    depth = gain_ref.shape[0]
    tail = depth - 6 * width
    o1, o2, o3 = (part.astype(jnp.float32) for part in split3(-offset))
    tail_id = lax.broadcasted_iota(jnp.int32, (tail, cols), 0)
    tail_rows = jnp.where(
        tail_id == 0, o1, jnp.where(tail_id == 1, o2, jnp.where(tail_id == 2, o3, 0.0))
    )
    gain_ref[6 * width :, :] = tail_rows.astype(jnp.bfloat16)

    x = xt_ref[...].T
    group = LANES // width
    x_wide = jnp.concatenate([x] * group, axis=1)
    x1, x2, x3 = (part.astype(jnp.float32) for part in split3(x_wide))
    lane = lax.broadcasted_iota(jnp.int32, (rows, LANES), 1)
    first_half = jnp.where(lane < 3 * width, x1, x2)
    second_half = jnp.where(
        lane < width, x2, jnp.where(lane < 2 * width, x3, jnp.where(lane < 2 * width + 3, 1.0, 0.0))
    )
    streamed = jnp.concatenate([first_half, second_half], axis=1).astype(jnp.bfloat16)

    quad_ref[...] = jnp.broadcast_to(start, (rows, LANES))
    tile_cols = 2 * LANES
    for t in range(cols // tile_cols):
        z = jnp.dot(
            streamed,
            gain_ref[:, t * tile_cols : (t + 1) * tile_cols],
            preferred_element_type=jnp.float32,
        )
        quad_ref[...] += z[:, :LANES] * z[:, :LANES] + z[:, LANES:] * z[:, LANES:]

    quad_t = quad_ref[...].T
    total = quad_t[:comps]
    for part in range(1, LANES // comps):
        total = total + quad_t[part * comps : (part + 1) * comps]
    log_dens = -0.5 * total
    peak = jnp.max(log_dens, axis=0, keepdims=True)
    weight = jnp.exp(log_dens - peak)
    norm = jnp.sum(weight, axis=0, keepdims=True)
    loglik = peak + jnp.log(norm)
    if loglik_ref is not None:
        for line in range(rows // LANES):
            loglik_ref[line : line + 1, :] = loglik[:, line * LANES : (line + 1) * LANES]
    respons = weight / norm
    resp_parts = jnp.concatenate(split3(respons), axis=0)

    center = jnp.mean(mu, axis=1, keepdims=True)
    yt_ref[...] = xt_ref[...] - center
    total_rows = feat_ref.shape[0] // 3

    def put(base, value):
        for place, part in enumerate(split3(value)):
            at = place * total_rows + base
            feat_ref[at : at + value.shape[0], :] = part

    products = []

    def product(i, c):
        return yt_ref[i : i + 1, :] * yt_ref[c * SUB : (c + 1) * SUB, :]

    for b, c in upper_pairs(width):
        products += [product(b * SUB + i, c) for i in range(SUB)]
    sub = lax.broadcasted_iota(jnp.int32, (SUB, rows), 0)
    for b, c in diagonal_pairs(width):
        products.append(product(b * SUB, b))
        for i in range(1, SUB):
            products.append(
                jnp.where(sub >= i, product(b * SUB + i, b), product(c * SUB + i - 1, c))
            )
        products.append(product(c * SUB + SUB - 1, c))
    for at in range(0, len(products), 2):
        put(at * SUB, jnp.concatenate(products[at : at + 2], axis=0))
    _, linear, ones, _ = moment_layout(width)
    put(linear, yt_ref[...])
    put(ones, jnp.ones((total_rows - ones, rows), jnp.float32))

    sums = lax.dot_general(
        feat_ref[...],
        resp_parts,
        (((1,), (1,)), ((), ())),
        preferred_element_type=jnp.float32,
    )
    sums = sums[:total_rows] + sums[total_rows : 2 * total_rows] + sums[2 * total_rows :]
    sums = sums[:, :comps] + sums[:, comps : 2 * comps] + sums[:, 2 * comps :]
    folds = LANES // comps
    part_rows = total_rows // folds
    packed = jnp.concatenate(
        [sums[place * part_rows : (place + 1) * part_rows] for place in range(folds)], axis=1
    )
    half = mine_ref.shape[0]
    core = own_half()
    lower, upper = packed[:half], packed[half:]
    mine_ref[...] = jnp.where(core == 0, lower, upper)
    other_ref[...] = jnp.where(core == 0, upper, lower)


def update(mine_ref, theirs_ref, mu, event_total):
    width, comps = mu.shape
    blocks = width // SUB
    core = own_half()
    mine, theirs = mine_ref[...], theirs_ref[...]
    packed = jnp.concatenate(
        [jnp.where(core == 0, mine, theirs), jnp.where(core == 0, theirs, mine)], axis=0
    )
    sums = jnp.concatenate(
        [packed[:, place * comps : (place + 1) * comps] for place in range(LANES // comps)], axis=0
    )
    diagonal, linear, ones, _ = moment_layout(width)
    about = sums[linear : linear + width]
    counts = sums[ones : ones + 1]

    shift = mu - jnp.mean(mu, axis=1, keepdims=True)
    first = about - counts * shift
    denom = counts + prior_count
    step = first / denom
    new_mu = mu + step
    new_logw = jnp.log(denom / (event_total + comps * prior_count))

    def block(value, b):
        return value[b * SUB : (b + 1) * SUB]

    def row(value, i):
        return jnp.broadcast_to(value[i : i + 1], (SUB, comps))

    sub_id = lax.broadcasted_iota(jnp.int32, (SUB, comps), 0)
    def register(place):
        return sums[place * SUB : (place + 1) * SUB]

    raw = {}
    for place, (b, c) in enumerate(upper_pairs(width)):
        for i in range(SUB):
            raw[b * SUB + i, c] = register(place * SUB + i)
    for place, (b, c) in enumerate(diagonal_pairs(width)):
        shared = [register(diagonal // SUB + place * (SUB + 1) + i) for i in range(SUB + 1)]
        for i in range(SUB):
            raw[b * SUB + i, b] = shared[i]
            value = shared[i + 1]
            for j in range(i + 1, SUB):
                value = jnp.where(sub_id == j, row(shared[j + 1], i), value)
            raw[c * SUB + i, c] = value

    cov = [dict() for _ in range(width)]
    for (at, c), value in raw.items():
        value = value - (
            row(about, at) * block(shift, c)
            + row(shift, at) * block(first, c)
            + row(first, at) * block(step, c)
        )
        if at // SUB == c:
            value = value + jnp.where(sub_id == at % SUB, ridge, 0.0)
        cov[at][c] = value

    inverse = [
        {i // SUB: jnp.where(sub_id == i % SUB, 1.0, 0.0).astype(jnp.float32)} for i in range(width)
    ]
    factors = []
    for p in range(width):
        b = p // SUB
        pivot = cov[p][b][p % SUB : p % SUB + 1]
        recip = jnp.broadcast_to(1.0 / pivot, (SUB, comps))
        scaled = {c: cov[p][c] * recip for c in range(b, blocks)}
        for i in range(p + 1, width):
            factor = row(scaled[i // SUB], i % SUB)
            for c in range(i // SUB, blocks):
                cov[i][c] = cov[i][c] - factor * cov[p][c]
            for c in range(b + 1):
                change = factor * inverse[p][c]
                inverse[i][c] = inverse[i][c] - change if c in inverse[i] else -change
        scale = jnp.broadcast_to(jnp.sqrt(denom / pivot), (SUB, comps))
        zero = jnp.zeros((SUB, comps), jnp.float32)
        factors.append(
            jnp.concatenate(
                [inverse[p][c] * scale if c in inverse[p] else zero for c in range(blocks)], axis=0
            )
        )
    return new_mu, factors, new_logw


def place_factors(proj_ref, rows_of, comps):
    group = LANES // comps
    for t in range(len(rows_of) // group):
        proj_ref[:, t * LANES : (t + 1) * LANES] = jnp.concatenate(
            rows_of[t * group : (t + 1) * group], axis=1
        )


def first_kernel(
    xt_hbm,
    factor_hbm,
    mu_hbm,
    logw_hbm,
    mine_ref,
    other_ref,
    xt_ref,
    sems,
    proj_ref,
    factor_ref,
    mu_ref,
    logw_ref,
    *scratch,
):
    pairs = ((factor_hbm, factor_ref), (mu_hbm, mu_ref), (logw_hbm, logw_ref), (xt_hbm, xt_ref))
    copies = [
        pltpu.make_async_copy(source, target, sems.at[place])
        for place, (source, target) in enumerate(pairs)
    ]
    for copy in copies:
        copy.start()
    for copy in copies:
        copy.wait()
    width, _, comps = factor_ref.shape
    place_factors(proj_ref, [factor_ref[i] for i in range(width)], comps)
    local_moments(
        xt_ref, proj_ref, mu_ref[...], logw_ref[...], None, mine_ref, other_ref, *scratch
    )


def middle_kernel(
    event_total,
    xt_ref,
    mine_ref,
    theirs_ref,
    mu_ref,
    loglik_ref,
    new_mine_ref,
    new_other_ref,
    new_mu_ref,
    proj_ref,
    *scratch,
):
    mu, factors, logw = update(mine_ref, theirs_ref, mu_ref[...], event_total)
    new_mu_ref[...] = mu
    place_factors(proj_ref, factors, mu.shape[1])
    local_moments(xt_ref, proj_ref, mu, logw, loglik_ref, new_mine_ref, new_other_ref, *scratch)


def last_kernel(
    event_total,
    mine_ref,
    theirs_ref,
    mu_ref,
    loglik_ref,
    new_mu_ref,
    factor_ref,
    logw_ref,
    loglik_out_ref,
):
    loglik_out_ref[...] = loglik_ref[...]
    mu, factors, logw = update(mine_ref, theirs_ref, mu_ref[...], event_total)
    new_mu_ref[...] = mu
    logw_ref[...] = logw
    for i, value in enumerate(factors):
        factor_ref[i] = value


def group_steps(size):
    steps, stride = [], 1
    while size > 1:
        radix = 4 if size % 4 == 0 else (2 if size % 2 == 0 else size)
        steps.append((stride, radix))
        stride *= radix
        size //= radix
    return steps


def peer(index, stride, radix, shift):
    digit = index // stride % radix
    other = digit ^ shift if radix & (radix - 1) == 0 else (digit + shift) % radix
    return index + (other - digit) * stride


def own_half():
    owner = lax.axis_index("comp")
    chip = lax.axis_index("dp")
    for stride, radix in group_steps(lax.axis_size("dp")):
        mask = crossing_mask(stride, radix)
        digit = chip // stride % radix
        for bit in (1, 2):
            if mask & bit:
                owner = owner + digit // bit % 2
    return owner % 2


def crossing_mask(stride, radix):
    if radix != 4:
        return 0
    return MASKS[0] if stride == 1 else MASKS[1]


def all_sum(mine, other):
    size = lax.axis_size("dp")
    cores = lax.axis_size("comp")
    swap = [(0, 1), (1, 0)]
    mine = mine + lax.ppermute(other, "comp", swap)
    for stride, radix in group_steps(size):
        order = list(range(1, radix))
        order = order[::-1] if stride == 1 else order[::2] + order[1::2]
        received = []
        for shift in order:
            flip = bin(shift & crossing_mask(stride, radix)).count("1") % 2
            pairs = [
                (i * cores + c, peer(i, stride, radix, shift) * cores + (c ^ flip))
                for i in range(size)
                for c in range(cores)
            ]
            received.append(lax.ppermute(mine, ("dp", "comp"), pairs))
        for value in received:
            mine = mine + value
    return mine, lax.ppermute(mine, "comp", swap)


def body(events, means, factors, log_weights):
    rows, width = events.shape
    comps = means.shape[0]
    event_total = rows * lax.axis_size("dp") * lax.axis_size("comp")
    cols = width * comps
    f32 = jnp.float32

    total_rows = moment_layout(width)[-1]
    halves = lax.axis_size("comp")
    mom_shape = jax.ShapeDtypeStruct((total_rows * comps // LANES // halves, LANES), f32)
    loglik_shape = jax.ShapeDtypeStruct((rows // LANES, LANES), f32)
    mu_shape = jax.ShapeDtypeStruct((width, comps), f32)
    scratch = [
        pltpu.VMEM((width, cols), f32),
        pltpu.VMEM((2 * LANES, cols), jnp.bfloat16),
        pltpu.VMEM((rows, LANES), f32),
        pltpu.VMEM((3 * total_rows, rows), jnp.bfloat16),
        pltpu.VMEM((width, rows), f32),
    ]
    load = [pltpu.VMEM((width, rows), f32), pltpu.SemaphoreType.DMA((4,))]
    params = pltpu.CompilerParams(vmem_limit_bytes=24 * 1024 * 1024)
    in_hbm = pl.BlockSpec(memory_space=pltpu.HBM)

    xt = events.T
    mu = means.T
    inputs = (xt, factors.transpose(1, 2, 0), mu, log_weights.reshape(1, comps))
    mine, other = pl.pallas_call(
        first_kernel,
        out_shape=(mom_shape, mom_shape),
        in_specs=[in_hbm] * 4,
        scratch_shapes=load
        + scratch[:1]
        + [
            pltpu.VMEM((width, width, comps), f32),
            pltpu.VMEM((width, comps), f32),
            pltpu.VMEM((1, comps), f32),
        ]
        + scratch[1:],
        compiler_params=params,
        name="first",
    )(*(pltpu.with_memory_space_constraint(value, pltpu.HBM) for value in inputs))
    for _ in range(1, ITERS):
        loglik, mine, other, mu = pl.pallas_call(
            functools.partial(middle_kernel, event_total),
            out_shape=(loglik_shape, mom_shape, mom_shape, mu_shape),
            scratch_shapes=scratch,
            compiler_params=params,
            name="middle",
        )(xt, *all_sum(mine, other), mu)
    mu, new_factors, logw, loglik = pl.pallas_call(
        functools.partial(last_kernel, event_total),
        out_shape=(
            mu_shape,
            jax.ShapeDtypeStruct((width, width, comps), f32),
            jax.ShapeDtypeStruct((1, comps), f32),
            loglik_shape,
        ),
        compiler_params=params,
        name="last",
    )(*all_sum(mine, other), mu, loglik)
    return mu.T, new_factors.transpose(2, 0, 1), logw.reshape(comps), loglik.reshape(rows)


def solution(mesh):
    in_specs = (P(("dp", "comp"), None), P(), P(), P())
    out_specs = (P(), P(), P(), P(("dp", "comp")))
    return jax.shard_map(body, mesh=mesh, in_specs=in_specs, out_specs=out_specs, check_vma=False)
```
